32 devices in a mesh: row: 8 (over z, x), col: 4 (over y, core).
Axes of the slice: x: 2, y: 2, z: 4, core: 2. Of those that a mesh axis runs over, the one named last changes fastest.
Arguments:
- field: bfloat16 [192, 128, 256], P('row', 'col'), may hold values from -6 to 6
- gains: float32 [1, 2, 256], replicated, may hold values from 0.5 to 1.5
- w_query: bfloat16 [1, 256, 256], replicated, may hold values from -24 to 24
- w_key: bfloat16 [1, 256, 256], replicated, may hold values from -1 to 1
- w_value: bfloat16 [1, 256, 256], replicated, may hold values from -0.375 to 0.375
- w_out: bfloat16 [1, 256, 256], replicated, may hold values from -0.375 to 0.375
- w_up: bfloat16 [1, 256, 1024], replicated, may hold values from -0.375 to 0.375
- w_down: bfloat16 [1, 1024, 256], replicated, may hold values from -0.1875 to 0.1875
- final_gain: float32 [256], replicated, may hold values from 0.5 to 1.5
- conv_weight: bfloat16 [3, 3, 256, 256], replicated, may hold values from -0.125 to 0.125
Outputs:
- image: float32 [16, 768, 512], P(None, 'row', 'col')
The draws below stay inside these ranges and needn't reach their ends.
All inputs are finite; a program needn't handle non-finite values.
Results may differ from the reference program's by a relative error of at most 0.0056.
Values may be sent and summed in bfloat16 or wider, within the bound.
A program may use at most 64 MiB of HBM per device.

```python
import jax
import jax.numpy as jnp
from jax import lax

D = 256
HEADS = 8
FF = 1024
HEAD = 32
WH = 24
WW = 32
HALO = 8
LAYERS = 1
OUT_CH = 16
SHUF = 4
ROWS = 192
COLS = 128


def query_and_key(key):
    base = jax.random.fold_in(key, 17)
    first, second = jax.random.split(base, 2)
    bound = min(3.0 * D ** (-0.5), 1.0)
    w_key = jnp.clip(jax.random.normal(first, (LAYERS, D, D), jnp.float32) * D ** (-0.5), -bound, bound)
    noise = jnp.clip(jax.random.normal(second, (LAYERS, D, D), jnp.float32) * D ** (-0.5), -bound, bound)
    w_query = noise
    return (w_query, w_key)


def draw_w_query(key, part):
    return query_and_key(key)[0].astype(jnp.bfloat16)


def draw_w_key(key, part):
    return query_and_key(key)[1].astype(jnp.bfloat16)


def shard_levels(own_key, shape, cuts, least, largest):
    level, own = 1.0, jax.random.fold_in(own_key, 6)
    for dim, blocks in cuts:
        draws = jnp.exp(jax.random.uniform(jax.random.fold_in(own, dim), (blocks,), jnp.float32, least / len(cuts), largest / len(cuts)))
        level = level * jnp.repeat(draws, shape[dim] // blocks).reshape([-1 if axis == dim else 1 for axis in range(len(shape))])
    return level


def centred(own_key, extent, deviation, most, cuts=(), held_as=jnp.bfloat16):
    values = deviation * jax.random.normal(own_key, extent, jnp.float32)
    if cuts:
        values = values * shard_levels(own_key, extent, cuts, -0.22, 0.18)
    return jnp.clip(values, -most, most).astype(held_as)


def setup_inputs(seed: int = 0) -> dict:
    splits = jax.random.split(jax.random.key(seed), 11)
    field = centred(splits[0], (ROWS, COLS, D), 1.0, 6.0, ((0, 8), (1, 4)))
    gains = jnp.clip(jax.random.uniform(splits[1], (LAYERS, 2, D), jnp.float32, 0.5, 1.5), 0.5, 1.5)
    w_query = draw_w_query(jax.random.fold_in(splits[10], 71), 0)
    w_key = draw_w_key(jax.random.fold_in(splits[10], 71), 0)
    w_value = centred(splits[4], (LAYERS, D, D), D ** -0.5, 0.375)
    w_out = centred(splits[5], (LAYERS, D, D), D ** -0.5, 0.375)
    w_up = centred(splits[6], (LAYERS, D, FF), D ** -0.5, 0.375)
    w_down = centred(splits[7], (LAYERS, FF, D), FF ** -0.5, 0.1875)
    final_gain = jnp.clip(jax.random.uniform(splits[8], (D,), jnp.float32, 0.5, 1.5), 0.5, 1.5)
    conv_weight = centred(splits[9], (3, 3, D, OUT_CH * SHUF * SHUF), (9 * D) ** -0.5, 0.125)
    return {"field": field, "gains": gains, "w_query": w_query, "w_key": w_key, "w_value": w_value, "w_out": w_out, "w_up": w_up, "w_down": w_down, "final_gain": final_gain, "conv_weight": conv_weight}


def rms(values, gain):
    return values * lax.rsqrt(lax.optimization_barrier(jnp.mean(values * values, axis=-1, keepdims=True)) + 1e-06) * gain

def attend(query, keys, values, valid):
    count = query.shape[0]
    width = keys.shape[0]
    q_heads = query.reshape(count, HEADS, HEAD).transpose(1, 0, 2)
    k_heads = keys.reshape(width, HEADS, HEAD).transpose(1, 0, 2)
    v_heads = values.reshape(width, HEADS, HEAD).transpose(1, 0, 2)

    def one_head(items):
        q_one, k_one, v_one = items
        scores = jnp.dot(q_one, k_one.T, preferred_element_type=jnp.float32) * HEAD ** (-0.5)
        scores = jnp.where(valid[None, :], scores, jnp.float32(-1e+30))
        top = lax.optimization_barrier(jnp.max(scores, axis=-1, keepdims=True))
        expo = jnp.exp(scores - top)
        weights = (expo / lax.optimization_barrier(jnp.sum(expo, axis=-1, keepdims=True))).astype(jnp.bfloat16)
        return jnp.dot(weights, v_one, preferred_element_type=jnp.float32)
    merged = lax.map(one_head, (q_heads, k_heads, v_heads))
    return merged.transpose(1, 0, 2).reshape(count, HEADS * HEAD).astype(jnp.bfloat16)

def reference(field, gains, w_query, w_key, w_value, w_out, w_up, w_down, final_gain, conv_weight):
    x = field.astype(jnp.float32)
    nrow = ROWS // WH
    ncol = COLS // WW
    pads = ((HALO, HALO), (HALO, HALO), (0, 0))
    validp = jnp.pad(jnp.ones((ROWS, COLS), jnp.float32), pads[:2]) > 0.5
    for layer in range(LAYERS):
        normed = rms(x, gains[layer, 0]).astype(jnp.bfloat16).reshape(-1, D)
        query = jnp.dot(normed, w_query[layer], preferred_element_type=jnp.float32).astype(jnp.bfloat16).reshape(ROWS, COLS, D)
        keys = jnp.dot(normed, w_key[layer], preferred_element_type=jnp.float32).astype(jnp.bfloat16).reshape(ROWS, COLS, D)
        values = jnp.dot(normed, w_value[layer], preferred_element_type=jnp.float32).astype(jnp.bfloat16).reshape(ROWS, COLS, D)
        keys_pad = jnp.pad(keys, pads)
        values_pad = jnp.pad(values, pads)

        def window(index):
            first = index // ncol * WH
            second = index % ncol * WW
            zero = jnp.zeros((), jnp.int32)
            q_block = lax.dynamic_slice(query, (first, second, zero), (WH, WW, D)).reshape(-1, D)
            k_block = lax.dynamic_slice(keys_pad, (first, second, zero), (WH + 2 * HALO, WW + 2 * HALO, D)).reshape(-1, D)
            v_block = lax.dynamic_slice(values_pad, (first, second, zero), (WH + 2 * HALO, WW + 2 * HALO, D)).reshape(-1, D)
            m_block = lax.dynamic_slice(validp, (first, second), (WH + 2 * HALO, WW + 2 * HALO)).reshape(-1)
            return attend(q_block, k_block, v_block, m_block)
        context = lax.map(window, jnp.arange(nrow * ncol, dtype=jnp.int32))
        context = context.reshape(nrow, ncol, WH, WW, D).transpose(0, 2, 1, 3, 4).reshape(-1, D)
        x = x + jnp.dot(context, w_out[layer], preferred_element_type=jnp.float32).reshape(ROWS, COLS, D)
        second_norm = rms(x, gains[layer, 1]).astype(jnp.bfloat16).reshape(-1, D)
        hidden = jax.nn.gelu(jnp.dot(second_norm, w_up[layer], preferred_element_type=jnp.float32)).astype(jnp.bfloat16)
        x = x + jnp.dot(hidden, w_down[layer], preferred_element_type=jnp.float32).reshape(ROWS, COLS, D)
    final = rms(x, final_gain).astype(jnp.bfloat16)
    padded = jnp.pad(final, ((1, 1), (1, 1), (0, 0)))
    conv = jnp.zeros((ROWS * COLS, OUT_CH * SHUF * SHUF), jnp.float32)
    for first in range(3):
        for second in range(3):
            piece = padded[first:first + ROWS, second:second + COLS].reshape(-1, D)
            conv = conv + jnp.dot(piece, conv_weight[first, second], preferred_element_type=jnp.float32)
    image = conv.reshape(ROWS, COLS, OUT_CH, SHUF, SHUF).transpose(2, 0, 3, 1, 4)
    return image.reshape(OUT_CH, ROWS * SHUF, COLS * SHUF)
```

```python
import functools

import jax
import jax.numpy as jnp
from jax import lax
from jax.experimental import pallas as pl
from jax.experimental.pallas import tpu as pltpu
from jax.sharding import PartitionSpec as P

HEADS = 8
HALO = 8
SHUF = 4
CHUNK = 256
STEP = 128
TAIL = 16
VMEM_LIMIT = 56 * 1024 * 1024
BF = jnp.bfloat16
F32 = jnp.float32
NEIGHBOURS = ((-1, 0), (1, 0), (0, -1), (0, 1), (-1, -1), (-1, 1), (1, -1), (1, 1))


def rms(values, gain):
    return values * lax.rsqrt(jnp.mean(values * values, axis=-1, keepdims=True) + 1e-06) * gain


def there(step, sizes):
    row, col = lax.axis_index("row"), lax.axis_index("col")
    nrow, ncol = row + step[0], col + step[1]
    ok = (nrow >= 0) & (nrow < sizes[0]) & (ncol >= 0) & (ncol < sizes[1])
    return ok, nrow, ncol


def greet(sizes):
    barrier = pltpu.get_barrier_semaphore()
    for step in NEIGHBOURS:
        ok, nrow, ncol = there(step, sizes)

        @pl.when(ok)
        def _():
            pl.semaphore_signal(
                barrier, inc=1, device_id=(nrow, ncol), device_id_type=pl.DeviceIdType.MESH
            )

    peers = jnp.int32(0)
    for step in NEIGHBOURS:
        peers = peers + there(step, sizes)[0].astype(jnp.int32)
    pl.semaphore_wait(barrier, peers)


def swap(sizes, sources, slots, send, recv, fills):
    copies = []
    for n, step in enumerate(NEIGHBOURS):
        ok, nrow, ncol = there(step, sizes)
        back = NEIGHBOURS.index((-step[0], -step[1]))
        copy = pltpu.make_async_remote_copy(
            src_ref=sources[n],
            dst_ref=slots[back],
            send_sem=send.at[n],
            recv_sem=recv.at[back],
            device_id=(nrow, ncol),
            device_id_type=pl.DeviceIdType.MESH,
        )
        arrival = pltpu.make_async_remote_copy(
            src_ref=slots[n],
            dst_ref=slots[n],
            send_sem=send.at[n],
            recv_sem=recv.at[n],
            device_id=(nrow, ncol),
            device_id_type=pl.DeviceIdType.MESH,
        )
        copies.append((ok, copy, arrival))
        pl.when(ok)(copy.start)
        pl.when(jnp.logical_not(ok))(fills[n])
    return copies


def finish(copies):
    for ok, copy, arrival in copies:
        pl.when(ok)(arrival.wait_recv)
    for ok, copy, _ in copies:
        pl.when(ok)(copy.wait_send)


def pieces(rows, groups):
    return [HALO * groups] * 2 + [rows] * 2 + [HALO] * 4


def halo_start(sizes, field_ref, halo_ref, send, recv):
    rows, groups = field_ref.shape[:2]
    sources, slots, fills = [], [], []
    first = 0
    for step, count in zip(NEIGHBOURS, pieces(rows, groups)):
        dr, dc = step
        rsel = slice(0, rows) if dr == 0 else (slice(0, HALO) if dr < 0 else slice(rows - HALO, rows))
        slot = halo_ref.at[pl.ds(first, count)]
        if dc == 0:
            sources.append(field_ref.at[rsel])
            slots.append(slot.reshape(HALO, groups, 8, field_ref.shape[3]))
        else:
            sources.append(field_ref.at[rsel, 0 if dc < 0 else groups - 1])
            slots.append(slot)

        def fill(first=first, count=count):
            for k in range(0, count, HALO):
                halo_ref[first + k : first + k + HALO] = field_ref[0:HALO, 0]

        fills.append(fill)
        first += count
    return swap(sizes, sources, slots, send, recv, fills)


def nt_dot(left, right):
    return lax.dot_general(left, right, (((1,), (1,)), ((), ())), preferred_element_type=F32)


def layer_kernel(
    sizes,
    field_ref, gains_ref, wq_ref, wk_ref, wv_ref, wo_hbm, wu_hbm, wd_hbm, fg_ref,
    out_ref, row_h, col_h, cor_h,
    halo_ref, qt_s, k_s, va_s, s_s, o_s, m_s, f_s, left_s, right_s, wo_ref, wu_ref, wd_ref,
    send, recv, send2, recv2, wsem,
):
    rows, groups = field_ref.shape[:2]
    cols = groups * 8
    width, tokens = qt_s.shape
    head = width // HEADS
    per = 128 // head
    loads = [
        pltpu.make_async_copy(src, dst, wsem.at[n])
        for n, (src, dst) in enumerate(((wo_hbm, wo_ref), (wu_hbm, wu_ref), (wd_hbm, wd_ref)))
    ]
    for load in loads:
        load.start()
    greet(sizes)
    copies = halo_start(sizes, field_ref, halo_ref, send, recv)

    g0 = gains_ref[0:1, :]
    g1 = gains_ref[1:2, :]
    fg = fg_ref[...]
    wqt = wq_ref[...].T
    wvt = wv_ref[...].T

    def keep(h, start, ok):
        count = h.shape[0]
        keys = slice(start, start + count)
        k_s[keys, :] = jnp.dot(h, wk_ref[...], preferred_element_type=F32).astype(BF)
        v = nt_dot(wvt, h)
        one = jnp.ones((TAIL, count), F32)
        if ok is not None:
            v = v * ok
            one = one * ok
        v = v.astype(BF)
        one = one.astype(BF)
        for e in range(HEADS):
            va_s[e, 0:head, keys] = v[e * head : (e + 1) * head]
            va_s[e, head : head + TAIL, keys] = one

    scale = head**-0.5 * 1.4426950408889634
    span = CHUNK // cols
    for start in range(0, tokens, CHUNK):
        at = start // cols
        h = rms(field_ref[at : at + span].astype(F32).reshape(CHUNK, width), g0).astype(BF)
        qt_s[:, start : start + CHUNK] = (nt_dot(wqt, h) * scale).astype(BF)
        keep(h, start, None)

    def scores(item, slot, first, count, base):
        start, e = item
        half, sub = e // per, e % per
        zero = jnp.zeros((head, CHUNK), BF)
        q = qt_s[e * head : (e + 1) * head, start : start + CHUNK]
        q = jnp.concatenate([q if n == sub else zero for n in range(per)], axis=0)
        top = base
        for kc in range(0, count, STEP):
            s = jnp.dot(
                k_s[first + kc : first + kc + STEP, half * 128 : half * 128 + 128], q,
                preferred_element_type=F32,
            )
            s_s[slot, kc : kc + STEP, :] = s
            part = jnp.max(s.reshape(STEP // 8, 8, CHUNK), axis=0)
            top = part if top is None else jnp.maximum(top, part)
            yield None
        top = jnp.max(top, axis=0, keepdims=True)
        yield top

    def values(item, slot, first, count, top):
        start, e = item
        acc = None
        for kc in range(0, count, STEP):
            p = jnp.exp2((s_s[slot, kc : kc + STEP, :] - top).astype(BF))
            o = jnp.dot(
                va_s[e, :, first + kc : first + kc + STEP], p, preferred_element_type=F32
            )
            acc = o if acc is None else acc + o
            yield None
        yield acc

    def attend(items, first, count, base, done):
        before = None
        for n, item in enumerate(items + [None]):
            slot = n % 2
            now = None if item is None else scores(item, slot, first, count, base(item))
            then = None if before is None else values(before[0], 1 - slot, first, count, before[1])
            top = acc = None
            for _ in range(count // STEP + 1):
                top = top if now is None else next(now)
                acc = acc if then is None else next(then)
            if before is not None:
                done(before[0], before[1], acc)
            before = (item, top)

    items = [(start, e) for start in range(0, tokens, CHUNK) for e in range(HEADS)]

    def own_done(item, top, acc):
        start, e = item
        o_s[e, :, start : start + CHUNK] = acc
        m_s[e, :, start : start + CHUNK] = jnp.broadcast_to(top, (8, CHUNK))

    attend(items, 0, tokens, lambda item: None, own_done)
    finish(copies)

    first = 0
    marks = []
    for step, count in zip(NEIGHBOURS, pieces(rows, groups)):
        ok = there(step, sizes)[0].astype(F32)
        marks.append((first * 8, count * 8, ok))
        first += count
    total = first * 8
    for start in range(0, total, 128):
        raw = halo_ref[start // 8 : start // 8 + 16].astype(F32).reshape(128, width)
        h = rms(raw, g0).astype(BF)
        spot = lax.broadcasted_iota(jnp.int32, (1, 128), 1) + start
        ok = jnp.zeros((1, 128), F32)
        for at, count, flag in marks:
            if at < start + 128 and at + count > start:
                ok = jnp.where((spot >= at) & (spot < at + count), flag, ok)
        keep(h, tokens + start, ok)
    for load in loads:
        load.wait()

    context = {}

    def tail(start, ctx):
        at = start // cols
        x = field_ref[at : at + span].astype(F32).reshape(CHUNK, width)
        x = x + jnp.dot(ctx, wo_ref[...], preferred_element_type=F32)
        h = rms(x, g1).astype(BF)
        u = jax.nn.gelu(jnp.dot(h, wu_ref[...], preferred_element_type=F32)).astype(BF)
        x = x + jnp.dot(u, wd_ref[...], preferred_element_type=F32)
        f = rms(x, fg)
        out_ref[at : at + span] = f.reshape(span, cols, width).astype(BF)
        for half in range(width // 128):
            f_s[half, start : start + CHUNK, :] = f[:, half * 128 : half * 128 + 128]

    def all_done(item, top, acc):
        start, e = item
        old = m_s[e, 0:1, start : start + CHUNK]
        acc = acc + o_s[e, :, start : start + CHUNK] * jnp.exp2(old - top)
        context[e] = acc[0:head] / acc[head : head + 1]
        if e == HEADS - 1:
            ctx = jnp.concatenate([context[n] for n in range(HEADS)], axis=0)
            tail(start, ctx.T.astype(BF))

    attend(
        items, tokens, total,
        lambda item: m_s[item[1], :, item[0] : item[0] + CHUNK], all_done,
    )
    for half in range(width // 128):
        sl = slice(half * 128, half * 128 + 128)
        left_s[:, sl] = f_s[half, pl.ds(0, rows, stride=cols), :].astype(BF)
        right_s[:, sl] = f_s[half, pl.ds(cols - 1, rows, stride=cols), :].astype(BF)
    slots = [row_h.at[0], row_h.at[1], col_h.at[0], col_h.at[1]] + [cor_h.at[n] for n in range(4)]
    sources = [
        out_ref.at[0], out_ref.at[rows - 1], left_s, right_s,
        left_s.at[pl.ds(0, 8)], right_s.at[pl.ds(0, 8)],
        left_s.at[pl.ds(rows - 8, 8)], right_s.at[pl.ds(rows - 8, 8)],
    ]

    def filler(slot):
        def fill():
            slot[...] = jnp.zeros(slot.shape, BF)
        return fill

    finish(swap(sizes, sources, slots, send2, recv2, [filler(s) for s in slots]))


def layer(sizes, field, gains, wq, wk, wv, wo, wu, wd, fg):
    rows, cols, width = field.shape
    groups = cols // 8
    tokens = rows * cols
    blocks = sum(pieces(rows, groups))
    keys = tokens + blocks * 8
    vm = pl.BlockSpec(memory_space=pltpu.VMEM)
    hbm = pl.BlockSpec(memory_space=pl.ANY)
    eight = pltpu.SemaphoreType.DMA((8,))
    return pl.pallas_call(
        functools.partial(layer_kernel, sizes),
        out_shape=(
            jax.ShapeDtypeStruct((rows, cols, width), BF),
            jax.ShapeDtypeStruct((2, cols, width), BF),
            jax.ShapeDtypeStruct((2, rows, width), BF),
            jax.ShapeDtypeStruct((4, 8, width), BF),
        ),
        in_specs=[vm] * 5 + [hbm] * 3 + [vm],
        out_specs=(vm,) * 4,
        scratch_shapes=[
            pltpu.VMEM((blocks, 8, width), BF),
            pltpu.VMEM((width, tokens), BF),
            pltpu.VMEM((keys, width), BF),
            pltpu.VMEM((HEADS, width // HEADS + TAIL, keys), BF),
            pltpu.VMEM((2, max(tokens, keys - tokens), CHUNK), F32),
            pltpu.VMEM((HEADS, width // HEADS + TAIL, tokens), F32),
            pltpu.VMEM((HEADS, 8, tokens), F32),
            pltpu.VMEM((width // 128, tokens, 128), F32),
            pltpu.VMEM((rows, width), BF),
            pltpu.VMEM((rows, width), BF),
            pltpu.VMEM(wo.shape, BF),
            pltpu.VMEM(wu.shape, BF),
            pltpu.VMEM(wd.shape, BF),
            eight, eight, eight, eight,
            pltpu.SemaphoreType.DMA((3,)),
        ],
        compiler_params=pltpu.CompilerParams(
            collective_id=0, has_side_effects=True, vmem_limit_bytes=VMEM_LIMIT
        ),
        name="layer",
    )(field.reshape(rows, groups, 8, width), gains, wq, wk, wv, wo, wu, wd, fg)


def conv_kernel(final_ref, row_h, col_h, cor_h, weight_ref, image_ref, fb_s, wp_s, up_s):
    rows, cols, width = final_ref.shape
    tokens = rows * cols
    outs = weight_ref.shape[1]
    old = lax.broadcasted_iota(jnp.int32, (outs, outs), 0)
    new = lax.broadcasted_iota(jnp.int32, (outs, outs), 1)
    want = (new % (outs // SHUF)) * SHUF + new // (outs // SHUF)
    perm = jnp.where(old == want, 1.0, 0.0).astype(BF)
    for tap in range(9):
        sl = slice(tap * width, (tap + 1) * width)
        wp_s[sl, :] = jnp.dot(weight_ref[sl, :], perm, preferred_element_type=F32).astype(BF)
    col = lax.broadcasted_iota(jnp.int32, (1, cols, 1), 1)

    def spread(first, count, x, before, after):
        flat = x.reshape(count * cols, width)
        low = pltpu.roll(flat, 1, 0).reshape(count, cols, width)
        high = pltpu.roll(flat, count * cols - 1, 0).reshape(count, cols, width)
        fb_s[1, first : first + count] = x.astype(BF)
        fb_s[0, first : first + count] = jnp.where(col == 0, before, low).astype(BF)
        fb_s[2, first : first + count] = jnp.where(col == cols - 1, after, high).astype(BF)

    for r in range(0, rows, 8):
        before = col_h[0, r : r + 8, :].astype(F32)[:, None, :]
        after = col_h[1, r : r + 8, :].astype(F32)[:, None, :]
        spread(1 + r, 8, final_ref[r : r + 8].astype(F32), before, after)
    for side, at, pick in ((0, 0, 7), (1, rows + 1, 0)):
        before = cor_h[2 * side].astype(F32)[pick : pick + 1][:, None, :]
        after = cor_h[2 * side + 1].astype(F32)[pick : pick + 1][:, None, :]
        spread(at, 1, row_h[side].astype(F32)[None], before, after)

    step = 8
    quarter = outs // SHUF
    for r in range(0, rows, step):
        acc = jnp.zeros((step * cols, outs), F32)
        for a in range(3):
            for b in range(3):
                tap = a * 3 + b
                acc = acc + jnp.dot(
                    fb_s[b, r + a : r + a + step].reshape(step * cols, width),
                    wp_s[tap * width : (tap + 1) * width, :],
                    preferred_element_type=F32,
                )
        for k in range(step):
            part = acc[k * cols : (k + 1) * cols]
            slot = k % 2
            for j in range(SHUF):
                pair = j * quarter // 128
                up_s[slot, pl.ds(j, cols, stride=SHUF), :] = part[:, pair * 128 : pair * 128 + 128]
            t = up_s[slot].T
            lanes = lax.broadcasted_iota(jnp.int32, (1, cols * SHUF), 1)
            t = jnp.where(lanes % 2 == 0, t[:quarter], t[quarter : 2 * quarter])
            for c in range(quarter // SHUF):
                image_ref[c, (r + k) * SHUF : (r + k + 1) * SHUF, :] = t[c * SHUF : (c + 1) * SHUF]


def conv_image(final, row, col, corner, weight):
    rows, cols, width = final.shape
    outs = weight.shape[1]
    vm = pl.BlockSpec(memory_space=pltpu.VMEM)
    return pl.pallas_call(
        conv_kernel,
        out_shape=jax.ShapeDtypeStruct((outs // SHUF**2, rows * SHUF, cols * SHUF), F32),
        in_specs=[vm] * 5,
        out_specs=vm,
        scratch_shapes=[
            pltpu.VMEM((3, rows + 2, cols, width), BF),
            pltpu.VMEM(weight.shape, BF),
            pltpu.VMEM((2, cols * SHUF, 128), F32),
        ],
        compiler_params=pltpu.CompilerParams(vmem_limit_bytes=VMEM_LIMIT),
        name="conv_image",
    )(final, row, col, corner, weight)


def local(sizes, field, gains, w_query, w_key, w_value, w_out, w_up, w_down, final_gain, conv_weight):
    final, row, col, corner = layer(
        sizes, field, gains[0], w_query[0], w_key[0], w_value[0], w_out[0], w_up[0], w_down[0],
        final_gain[None, :],
    )
    weight = conv_weight.reshape(-1, conv_weight.shape[3])
    return conv_image(final, row, col, corner, weight)


def solution(mesh):
    sizes = (mesh.shape["row"], mesh.shape["col"])
    return jax.shard_map(
        functools.partial(local, sizes),
        mesh=mesh,
        in_specs=(P("row", "col", None), P(), P(), P(), P(), P(), P(), P(), P(), P()),
        out_specs=P(None, "row", "col"),
        check_vma=False,
    )
```

```python
import functools

import jax
import jax.numpy as jnp
from jax import lax
from jax.experimental import pallas as pl
from jax.experimental.pallas import tpu as pltpu
from jax.sharding import PartitionSpec as P

HEADS = 8
HALO = 8
SHUF = 4
CHUNK = 256
STEP = 384
TAIL = 16
VMEM_LIMIT = 24 * 1024 * 1024
BF = jnp.bfloat16
F32 = jnp.float32
NEIGHBOURS = ((0, -1), (0, 1), (-1, 0), (1, 0), (-1, -1), (-1, 1), (1, -1), (1, 1))


def rms(values, gain):
    return values * lax.rsqrt(jnp.mean(values * values, axis=-1, keepdims=True) + 1e-06) * gain


def there(step, sizes):
    row, col = lax.axis_index("row"), lax.axis_index("col")
    nrow, ncol = row + step[0], col + step[1]
    ok = (nrow >= 0) & (nrow < sizes[0]) & (ncol >= 0) & (ncol < sizes[1])
    return ok, nrow, ncol


def greet(sizes):
    barrier = pltpu.get_barrier_semaphore()
    for step in NEIGHBOURS:
        ok, nrow, ncol = there(step, sizes)

        @pl.when(ok)
        def _():
            pl.semaphore_signal(
                barrier, inc=1, device_id=(nrow, ncol), device_id_type=pl.DeviceIdType.MESH
            )

    peers = jnp.int32(0)
    for step in NEIGHBOURS:
        peers = peers + there(step, sizes)[0].astype(jnp.int32)
    pl.semaphore_wait(barrier, peers)


def swap(sizes, sources, slots, send, recv, fills):
    copies = []
    for n, step in enumerate(NEIGHBOURS):
        ok, nrow, ncol = there(step, sizes)
        back = NEIGHBOURS.index((-step[0], -step[1]))
        copy = pltpu.make_async_remote_copy(
            src_ref=sources[n],
            dst_ref=slots[back],
            send_sem=send.at[n],
            recv_sem=recv.at[back],
            device_id=(nrow, ncol),
            device_id_type=pl.DeviceIdType.MESH,
        )
        arrival = pltpu.make_async_remote_copy(
            src_ref=slots[n],
            dst_ref=slots[n],
            send_sem=send.at[n],
            recv_sem=recv.at[n],
            device_id=(nrow, ncol),
            device_id_type=pl.DeviceIdType.MESH,
        )
        copies.append((ok, copy, arrival))
        pl.when(ok)(copy.start)
        if fills is not None:
            pl.when(jnp.logical_not(ok))(fills[n])
    return copies


def arrive(copies):
    for ok, _, arrival in copies:
        pl.when(ok)(arrival.wait_recv)


def leave(copies):
    for ok, copy, _ in copies:
        pl.when(ok)(copy.wait_send)


def pieces(rows, groups):
    return [rows] * 2 + [HALO * groups] * 2 + [HALO] * 4


def halo_start(sizes, field_ref, halo_ref, send, recv):
    rows, groups = field_ref.shape[:2]
    sources, slots, fills = [], [], []
    first = 0
    for step, count in zip(NEIGHBOURS, pieces(rows, groups)):
        dr, dc = step
        rsel = slice(0, rows) if dr == 0 else (slice(0, HALO) if dr < 0 else slice(rows - HALO, rows))
        slot = halo_ref.at[pl.ds(first, count)]
        if dc == 0:
            sources.append(field_ref.at[rsel])
            slots.append(slot.reshape(HALO, groups, 8, field_ref.shape[3]))
        else:
            sources.append(field_ref.at[rsel, 0 if dc < 0 else groups - 1])
            slots.append(slot)

        def fill(first=first, count=count):
            for k in range(0, count, HALO):
                halo_ref[first + k : first + k + HALO] = field_ref[0:HALO, 0]

        fills.append(fill)
        first += count
    return swap(sizes, sources, slots, send, recv, fills)


def nt_dot(left, right):
    return lax.dot_general(left, right, (((1,), (1,)), ((), ())), preferred_element_type=F32)


def layer_kernel(
    sizes,
    field_hbm, gains_hbm, wq_hbm, wk_hbm, wv_hbm, wo_hbm, wu_hbm, wd_hbm, fg_hbm,
    out_ref, row_h, col_h, cor_h,
    field_ref, gains_ref, wq_ref, wk_ref, wv_ref, wo_ref, wu_ref, wd_ref, fg_ref,
    halo_ref, qt_s, k_s, va_s, s_s, o_s, m_s, f_s, left_s, right_s,
    send, recv, send2, recv2, wsem,
):
    rows, groups = field_ref.shape[:2]
    width, tokens = qt_s.shape
    head = width // HEADS
    per = 128 // head
    loads = [
        pltpu.make_async_copy(src, dst, wsem.at[n])
        for n, (src, dst) in enumerate((
            (field_hbm, field_ref), (gains_hbm, gains_ref), (wq_hbm, wq_ref), (wk_hbm, wk_ref),
            (wv_hbm, wv_ref), (wo_hbm, wo_ref), (wu_hbm, wu_ref), (wd_hbm, wd_ref),
            (fg_hbm, fg_ref),
        ))
    ]
    for load in loads:
        load.start()
    for slot in (row_h, col_h, cor_h):
        slot[...] = jnp.zeros(slot.shape, BF)
    greet(sizes)
    loads[0].wait()
    copies = halo_start(sizes, field_ref, halo_ref, send, recv)
    for load in loads[1:]:
        load.wait()

    g0 = gains_ref[0:1, :]
    g1 = gains_ref[1:2, :]
    fg = fg_ref[...]
    wqt = wq_ref[...].T
    wvt = wv_ref[...].T

    def edge(spot):
        return spot[0] in (0, rows - 1) or spot[1] in (0, groups - 1)

    spots = [(r, g) for r in range(rows) for g in range(groups)]
    spots = [spot for spot in spots if edge(spot)] + [spot for spot in spots if not edge(spot)]
    lot = CHUNK // 8
    edges = sum(edge(spot) for spot in spots)
    starts = list(range(0, tokens, CHUNK))
    ready = max(start for start in starts if start < edges * 8)

    def take(start):
        part = spots[start // 8 : start // 8 + lot]
        return jnp.concatenate([field_ref[r, g].astype(F32) for r, g in part], axis=0)

    def keep(h, start, ok):
        count = h.shape[0]
        keys = slice(start, start + count)
        k_s[keys, :] = jnp.dot(h, wk_ref[...], preferred_element_type=F32).astype(BF)
        v = nt_dot(wvt, h)
        one = jnp.ones((TAIL, count), F32)
        if ok is not None:
            v = v * ok
            one = one * ok
        v = v.astype(BF)
        one = one.astype(BF)
        for e in range(HEADS):
            va_s[e, 0:head, keys] = v[e * head : (e + 1) * head]
            va_s[e, head : head + TAIL, keys] = one

    scale = head**-0.5 * 1.4426950408889634
    for start in starts:
        h = rms(take(start), g0).astype(BF)
        qt_s[:, start : start + CHUNK] = (nt_dot(wqt, h) * scale).astype(BF)
        keep(h, start, None)

    def scores(item, slot, first, count, base):
        start, e = item
        half, sub = e // per, e % per
        zero = jnp.zeros((head, CHUNK), BF)
        q = qt_s[e * head : (e + 1) * head, start : start + CHUNK]
        q = jnp.concatenate([q if n == sub else zero for n in range(per)], axis=0)
        top = base
        for kc in range(0, count, STEP):
            s = jnp.dot(
                k_s[first + kc : first + kc + STEP, half * 128 : half * 128 + 128], q,
                preferred_element_type=F32,
            )
            s_s[slot, kc : kc + STEP, :] = s
            part = jnp.max(s.reshape(STEP // 8, 8, CHUNK), axis=0)
            top = part if top is None else jnp.maximum(top, part)
            yield None
        top = jnp.max(top, axis=0, keepdims=True)
        yield top

    def values(item, slot, first, count, top):
        start, e = item
        acc = None
        for kc in range(0, count, STEP):
            p = jnp.exp2((s_s[slot, kc : kc + STEP, :] - top).astype(BF))
            o = jnp.dot(
                va_s[e, :, first + kc : first + kc + STEP], p, preferred_element_type=F32
            )
            acc = o if acc is None else acc + o
            yield None
        yield acc

    items = [(start, e) for start in starts for e in range(HEADS)]

    def attend(first, count, base, done):
        before = None
        for n, item in enumerate(items + [None]):
            slot = n % 2
            now = None if item is None else scores(item, slot, first, count, base(item))
            then = None if before is None else values(before[0], 1 - slot, first, count, before[1])
            top = acc = None
            for _ in range(count // STEP + 1):
                top = top if now is None else next(now)
                acc = acc if then is None else next(then)
            if before is not None:
                done(before[0], before[1], acc)
            before = (item, top)

    def put(item, top, acc):
        start, e = item
        o_s[e, :, start : start + CHUNK] = acc
        m_s[e, :, start : start + CHUNK] = jnp.broadcast_to(top, (8, CHUNK))

    def join(item, top, acc):
        start, e = item
        old = m_s[e, 0:1, start : start + CHUNK]
        return acc + o_s[e, :, start : start + CHUNK] * jnp.exp2(old - top)

    def held(item):
        return m_s[item[1], :, item[0] : item[0] + CHUNK]

    marks = []
    first = 0
    for step, count in zip(NEIGHBOURS, pieces(rows, groups)):
        marks.append((first * 8, count * 8, there(step, sizes)[0].astype(F32)))
        first += count
    total = first * 8
    sides = 2 * rows * 8

    def halo_keys(begin, end, size):
        for start in range(begin, end, size):
            raw = halo_ref[start // 8 : (start + size) // 8].astype(F32).reshape(size, width)
            h = rms(raw, g0).astype(BF)
            spot = lax.broadcasted_iota(jnp.int32, (1, size), 1) + start
            ok = jnp.zeros((1, size), F32)
            for at, count, flag in marks:
                if at < start + size and at + count > start:
                    ok = jnp.where((spot >= at) & (spot < at + count), flag, ok)
            keep(h, tokens + start, ok)

    attend(0, tokens, lambda item: None, put)
    arrive(copies[:2])
    halo_keys(0, sides, 128)
    attend(tokens, sides, held, lambda item, top, acc: put(item, top, join(item, top, acc)))
    arrive(copies[2:])
    halo_keys(sides, total, 256)

    def tail(start, ctx):
        x = take(start)
        x = x + jnp.dot(ctx, wo_ref[...], preferred_element_type=F32)
        h = rms(x, g1).astype(BF)
        u = jax.nn.gelu(jnp.dot(h, wu_ref[...], preferred_element_type=F32)).astype(BF)
        x = x + jnp.dot(u, wd_ref[...], preferred_element_type=F32)
        f = rms(x, fg)
        for n, (r, g) in enumerate(spots[start // 8 : start // 8 + lot]):
            piece = f[n * 8 : n * 8 + 8]
            out_ref[r, g] = piece.astype(BF)
            for side, where in ((0, 0), (1, groups - 1)):
                if g == where:
                    for half in range(width // 128):
                        f_s[side, half, r * 8 : r * 8 + 8, :] = piece[:, half * 128 : half * 128 + 128]

    slots = [col_h.at[0], col_h.at[1], row_h.at[0], row_h.at[1]] + [cor_h.at[n] for n in range(4)]
    sources = [
        left_s, right_s, out_ref.at[0], out_ref.at[rows - 1],
        left_s.at[pl.ds(0, 8)], right_s.at[pl.ds(0, 8)],
        left_s.at[pl.ds(rows - 8, 8)], right_s.at[pl.ds(rows - 8, 8)],
    ]
    context = {}
    final = []

    def finals(item, top, acc):
        start, e = item
        acc = join(item, top, acc)
        context[e] = acc[0:head] / acc[head : head + 1]
        if e == HEADS - 1:
            ctx = jnp.concatenate([context[n] for n in range(HEADS)], axis=0)
            tail(start, ctx.T.astype(BF))
            if start == ready:
                for half in range(width // 128):
                    sl = slice(half * 128, half * 128 + 128)
                    left_s[:, sl] = f_s[0, half, pl.ds(0, rows, stride=8), :].astype(BF)
                    right_s[:, sl] = f_s[1, half, pl.ds(7, rows, stride=8), :].astype(BF)
                final.extend(swap(sizes, sources, slots, send2, recv2, None))

    attend(tokens + sides, total - sides, held, finals)
    leave(copies)
    arrive(final)
    leave(final)


def layer(sizes, field, gains, wq, wk, wv, wo, wu, wd, fg):
    rows, cols, width = field.shape
    groups = cols // 8
    tokens = rows * cols
    blocks = sum(pieces(rows, groups))
    keys = tokens + blocks * 8
    aug = width // HEADS + TAIL
    vm = pl.BlockSpec(memory_space=pltpu.VMEM)
    hbm = pl.BlockSpec(memory_space=pltpu.HBM)
    eight = pltpu.SemaphoreType.DMA((8,))
    field = field.reshape(rows, groups, 8, width)
    inputs = (field, gains, wq, wk, wv, wo, wu, wd, fg)
    inputs = tuple(pltpu.with_memory_space_constraint(a, pltpu.HBM) for a in inputs)
    final, row, col, corner = pl.pallas_call(
        functools.partial(layer_kernel, sizes),
        out_shape=(
            jax.ShapeDtypeStruct((rows, groups, 8, width), BF),
            jax.ShapeDtypeStruct((2, groups, 8, width), BF),
            jax.ShapeDtypeStruct((2, rows, width), BF),
            jax.ShapeDtypeStruct((4, 8, width), BF),
        ),
        in_specs=[hbm] * len(inputs),
        out_specs=(vm,) * 4,
        scratch_shapes=[pltpu.VMEM(a.shape, a.dtype) for a in inputs] + [
            pltpu.VMEM((blocks, 8, width), BF),
            pltpu.VMEM((width, tokens), BF),
            pltpu.VMEM((keys, width), BF),
            pltpu.VMEM((HEADS, aug, keys), BF),
            pltpu.VMEM((2, tokens, CHUNK), F32),
            pltpu.VMEM((HEADS, aug, tokens), F32),
            pltpu.VMEM((HEADS, 8, tokens), F32),
            pltpu.VMEM((2, width // 128, rows * 8, 128), F32),
            pltpu.VMEM((rows, width), BF),
            pltpu.VMEM((rows, width), BF),
            eight, eight, eight, eight,
            pltpu.SemaphoreType.DMA((len(inputs),)),
        ],
        compiler_params=pltpu.CompilerParams(
            collective_id=0, has_side_effects=True, vmem_limit_bytes=VMEM_LIMIT,
        ),
        name="layer",
    )(*inputs)
    return final.reshape(rows, cols, width), row.reshape(2, cols, width), col, corner


def conv_kernel(final_ref, row_h, col_h, cor_h, weight_ref, image_hbm, image_ref, fb_s, wp_s, up_s, sem):
    rows, cols, width = final_ref.shape
    tokens = rows * cols
    outs = weight_ref.shape[1]
    old = lax.broadcasted_iota(jnp.int32, (outs, outs), 0)
    new = lax.broadcasted_iota(jnp.int32, (outs, outs), 1)
    want = (new % (outs // SHUF)) * SHUF + new // (outs // SHUF)
    perm = jnp.where(old == want, 1.0, 0.0).astype(BF)
    for tap in range(9):
        sl = slice(tap * width, (tap + 1) * width)
        wp_s[sl, :] = jnp.dot(weight_ref[sl, :], perm, preferred_element_type=F32).astype(BF)
    col = lax.broadcasted_iota(jnp.int32, (1, cols, 1), 1)

    def spread(first, count, x, before, after):
        flat = x.reshape(count * cols, width)
        low = pltpu.roll(flat, 1, 0).reshape(count, cols, width)
        high = pltpu.roll(flat, count * cols - 1, 0).reshape(count, cols, width)
        fb_s[1, first : first + count] = x.astype(BF)
        fb_s[0, first : first + count] = jnp.where(col == 0, before, low).astype(BF)
        fb_s[2, first : first + count] = jnp.where(col == cols - 1, after, high).astype(BF)

    for r in range(0, rows, 8):
        before = col_h[0, r : r + 8, :].astype(F32)[:, None, :]
        after = col_h[1, r : r + 8, :].astype(F32)[:, None, :]
        spread(1 + r, 8, final_ref[r : r + 8].astype(F32), before, after)
    for side, at, pick in ((0, 0, 7), (1, rows + 1, 0)):
        before = cor_h[2 * side].astype(F32)[pick : pick + 1][:, None, :]
        after = cor_h[2 * side + 1].astype(F32)[pick : pick + 1][:, None, :]
        spread(at, 1, row_h[side].astype(F32)[None], before, after)

    step = 8
    quarter = outs // SHUF
    outs_going = []
    for r in range(0, rows, step):
        acc = jnp.zeros((step * cols, outs), F32)
        for a in range(3):
            for b in range(3):
                tap = a * 3 + b
                acc = acc + jnp.dot(
                    fb_s[b, r + a : r + a + step].reshape(step * cols, width),
                    wp_s[tap * width : (tap + 1) * width, :],
                    preferred_element_type=F32,
                )
        for k in range(step):
            part = acc[k * cols : (k + 1) * cols]
            slot = k % 2
            for j in range(SHUF):
                pair = j * quarter // 128
                up_s[slot, pl.ds(j, cols, stride=SHUF), :] = part[:, pair * 128 : pair * 128 + 128]
            t = up_s[slot].T
            lanes = lax.broadcasted_iota(jnp.int32, (1, cols * SHUF), 1)
            t = jnp.where(lanes % 2 == 0, t[:quarter], t[quarter : 2 * quarter])
            for c in range(quarter // SHUF):
                image_ref[c, (r + k) * SHUF : (r + k + 1) * SHUF, :] = t[c * SHUF : (c + 1) * SHUF]
        band = pl.ds(r * SHUF, step * SHUF)
        outs_going.append(pltpu.make_async_copy(
            image_ref.at[:, band], image_hbm.at[:, band], sem.at[r // step]
        ))
        outs_going[-1].start()
    for going in outs_going:
        going.wait()


def conv_image(final, row, col, corner, weight):
    rows, cols, width = final.shape
    outs = weight.shape[1]
    vm = pl.BlockSpec(memory_space=pltpu.VMEM)
    return pl.pallas_call(
        conv_kernel,
        out_shape=jax.ShapeDtypeStruct((outs // SHUF**2, rows * SHUF, cols * SHUF), F32),
        in_specs=[vm] * 5,
        out_specs=pl.BlockSpec(memory_space=pltpu.HBM),
        scratch_shapes=[
            pltpu.VMEM((outs // SHUF**2, rows * SHUF, cols * SHUF), F32),
            pltpu.VMEM((3, rows + 2, cols, width), BF),
            pltpu.VMEM(weight.shape, BF),
            pltpu.VMEM((2, cols * SHUF, 128), F32),
            pltpu.SemaphoreType.DMA((rows // 8,)),
        ],
        compiler_params=pltpu.CompilerParams(vmem_limit_bytes=VMEM_LIMIT),
        name="conv_image",
    )(final, row, col, corner, weight)


def local(sizes, field, gains, w_query, w_key, w_value, w_out, w_up, w_down, final_gain, conv_weight):
    final, row, col, corner = layer(
        sizes, field, gains[0], w_query[0], w_key[0], w_value[0], w_out[0], w_up[0], w_down[0],
        final_gain[None, :],
    )
    weight = conv_weight.reshape(-1, conv_weight.shape[3])
    return conv_image(final, row, col, corner, weight)


def solution(mesh):
    sizes = (mesh.shape["row"], mesh.shape["col"])
    return jax.shard_map(
        functools.partial(local, sizes),
        mesh=mesh,
        in_specs=(P("row", "col", None), P(), P(), P(), P(), P(), P(), P(), P(), P()),
        out_specs=P(None, "row", "col"),
        check_vma=False,
    )
```

```python
import functools

import jax
import jax.numpy as jnp
from jax import lax
from jax.experimental import pallas as pl
from jax.experimental.pallas import tpu as pltpu
from jax.sharding import PartitionSpec as P

HEADS = 8
HALO = 8
SHUF = 4
CHUNK = 256
TAIL = 16
VMEM_LIMIT = 24 * 1024 * 1024
BF = jnp.bfloat16
F32 = jnp.float32
NEIGHBOURS = ((0, -1), (0, 1), (-1, 0), (1, 0), (-1, -1), (-1, 1), (1, -1), (1, 1))


def rms(values, gain):
    return values * lax.rsqrt(jnp.mean(values * values, axis=-1, keepdims=True) + 1e-06) * gain


def there(step, sizes):
    row, col = lax.axis_index("row"), lax.axis_index("col")
    nrow, ncol = row + step[0], col + step[1]
    ok = (nrow >= 0) & (nrow < sizes[0]) & (ncol >= 0) & (ncol < sizes[1])
    return ok, nrow, ncol


def greet(sizes):
    barrier = pltpu.get_barrier_semaphore()
    for step in NEIGHBOURS:
        ok, nrow, ncol = there(step, sizes)

        @pl.when(ok)
        def _():
            pl.semaphore_signal(
                barrier, inc=1, device_id=(nrow, ncol), device_id_type=pl.DeviceIdType.MESH
            )

    peers = jnp.int32(0)
    for step in NEIGHBOURS:
        peers = peers + there(step, sizes)[0].astype(jnp.int32)
    pl.semaphore_wait(barrier, peers)


def swap(sizes, sources, slots, send, recv, fills):
    copies = []
    for n, step in enumerate(NEIGHBOURS):
        ok, nrow, ncol = there(step, sizes)
        back = NEIGHBOURS.index((-step[0], -step[1]))
        copy = pltpu.make_async_remote_copy(
            src_ref=sources[n],
            dst_ref=slots[back],
            send_sem=send.at[n],
            recv_sem=recv.at[back],
            device_id=(nrow, ncol),
            device_id_type=pl.DeviceIdType.MESH,
        )
        arrival = pltpu.make_async_remote_copy(
            src_ref=slots[n],
            dst_ref=slots[n],
            send_sem=send.at[n],
            recv_sem=recv.at[n],
            device_id=(nrow, ncol),
            device_id_type=pl.DeviceIdType.MESH,
        )
        copies.append((ok, copy, arrival))
        pl.when(ok)(copy.start)
        if fills is not None:
            pl.when(jnp.logical_not(ok))(fills[n])
    return copies


def arrive(copies):
    for ok, _, arrival in copies:
        pl.when(ok)(arrival.wait_recv)


def leave(copies):
    for ok, copy, _ in copies:
        pl.when(ok)(copy.wait_send)


def pieces(rows, groups):
    return [rows] * 2 + [HALO * groups] * 2 + [HALO] * 4


def halo_start(sizes, field_ref, halo_ref, send, recv):
    rows, groups = field_ref.shape[:2]
    sources, slots, fills = [], [], []
    first = 0
    for step, count in zip(NEIGHBOURS, pieces(rows, groups)):
        dr, dc = step
        rsel = slice(0, rows) if dr == 0 else (slice(0, HALO) if dr < 0 else slice(rows - HALO, rows))
        slot = halo_ref.at[pl.ds(first, count)]
        if dc == 0:
            sources.append(field_ref.at[rsel])
            slots.append(slot.reshape(HALO, groups, 8, field_ref.shape[3]))
        else:
            sources.append(field_ref.at[rsel, 0 if dc < 0 else groups - 1])
            slots.append(slot)

        def fill(first=first, count=count):
            for k in range(0, count, HALO):
                halo_ref[first + k : first + k + HALO] = field_ref[0:HALO, 0]

        fills.append(fill)
        first += count
    return swap(sizes, sources, slots, send, recv, fills)


def nt_dot(left, right):
    return lax.dot_general(left, right, (((1,), (1,)), ((), ())), preferred_element_type=F32)


def layer_kernel(
    sizes,
    field_hbm, gains_hbm, wq_hbm, wk_hbm, wv_hbm, wo_hbm, wu_hbm, wd_hbm, fg_hbm,
    out_ref, row_h, col_h, cor_h,
    field_ref, gains_ref, wq_ref, wk_ref, wv_ref, wo_ref, wu_ref, wd_ref, fg_ref,
    halo_ref, qt_s, k_s, va_s, s_s, o_s, m_s, f_s, left_s, right_s,
    send, recv, send2, recv2, wsem,
):
    rows, groups = field_ref.shape[:2]
    width, tokens = qt_s.shape
    head = width // HEADS
    per = 128 // head
    loads = [
        pltpu.make_async_copy(src, dst, wsem.at[n])
        for n, (src, dst) in enumerate((
            (field_hbm, field_ref), (gains_hbm, gains_ref), (wq_hbm, wq_ref), (wk_hbm, wk_ref),
            (wv_hbm, wv_ref), (wo_hbm, wo_ref), (wu_hbm, wu_ref), (wd_hbm, wd_ref),
            (fg_hbm, fg_ref),
        ))
    ]
    for load in loads:
        load.start()
    for slot in (row_h, col_h, cor_h):
        slot[...] = jnp.zeros(slot.shape, BF)
    greet(sizes)
    loads[0].wait()
    copies = halo_start(sizes, field_ref, halo_ref, send, recv)
    for load in loads[1:]:
        load.wait()

    g0 = gains_ref[0:1, :]
    g1 = gains_ref[1:2, :]
    fg = fg_ref[...]
    wqt = wq_ref[...].T
    wvt = wv_ref[...].T

    def edge(spot):
        return spot[0] in (0, rows - 1) or spot[1] in (0, groups - 1)

    spots = [(r, g) for r in range(rows) for g in range(groups)]
    spots = [spot for spot in spots if edge(spot)] + [spot for spot in spots if not edge(spot)]
    lot = CHUNK // 8
    edges = sum(edge(spot) for spot in spots)
    starts = list(range(0, tokens, CHUNK))
    ready = max(start for start in starts if start < edges * 8)

    def take(start):
        part = spots[start // 8 : start // 8 + lot]
        return jnp.concatenate([field_ref[r, g].astype(F32) for r, g in part], axis=0)

    def keep(h, start, ok):
        count = h.shape[0]
        keys = slice(start, start + count)
        k_s[keys, :] = jnp.dot(h, wk_ref[...], preferred_element_type=F32).astype(BF)
        v = nt_dot(wvt, h)
        one = jnp.ones((TAIL, count), F32)
        if ok is not None:
            v = v * ok
            one = one * ok
        v = v.astype(BF)
        one = one.astype(BF)
        for e in range(HEADS):
            va_s[e, 0:head, keys] = v[e * head : (e + 1) * head]
            va_s[e, head : head + TAIL, keys] = one

    scale = head**-0.5 * 1.4426950408889634
    for start in starts:
        h = rms(take(start), g0).astype(BF)
        qt_s[:, start : start + CHUNK] = (nt_dot(wqt, h) * scale).astype(BF)
        keep(h, start, None)

    def scores(item, slot, first, count, step, base):
        start, e = item
        half, sub = e // per, e % per
        zero = jnp.zeros((head, CHUNK), BF)
        q = qt_s[e * head : (e + 1) * head, start : start + CHUNK]
        q = jnp.concatenate([q if n == sub else zero for n in range(per)], axis=0)
        top = base
        for kc in range(0, count, step):
            s = jnp.dot(
                k_s[first + kc : first + kc + step, half * 128 : half * 128 + 128], q,
                preferred_element_type=F32,
            )
            s_s[slot, kc : kc + step, :] = s
            part = jnp.max(s.reshape(step // 8, 8, CHUNK), axis=0)
            top = part if top is None else jnp.maximum(top, part)
            yield None
        yield jnp.max(top, axis=0, keepdims=True)

    def values(item, slot, first, count, step, top):
        start, e = item
        acc = None
        for kc in range(0, count, step):
            p = jnp.exp2((s_s[slot, kc : kc + step, :] - top).astype(BF))
            o = jnp.dot(
                va_s[e, :, first + kc : first + kc + step], p, preferred_element_type=F32
            )
            acc = o if acc is None else acc + o
            yield None
        yield acc

    items = [(start, e) for start in starts for e in range(HEADS)]

    def attend(first, count, step, lag, base, done):
        tops = {}
        for n in range(len(items) + lag):
            old = n - lag
            now = then = top = acc = None
            if n < len(items):
                now = scores(items[n], n % (lag + 1), first, count, step, base(items[n]))
            if old >= 0:
                then = values(items[old], old % (lag + 1), first, count, step, tops[old])
            for _ in range(count // step + 1):
                top = top if now is None else next(now)
                acc = acc if then is None else next(then)
            tops[n] = top
            if old >= 0:
                done(items[old], tops.pop(old), acc)

    def put(item, top, acc):
        start, e = item
        o_s[e, :, start : start + CHUNK] = acc
        m_s[e, :, start : start + CHUNK] = jnp.broadcast_to(top, (8, CHUNK))

    def join(item, top, acc):
        start, e = item
        old = m_s[e, 0:1, start : start + CHUNK]
        return acc + o_s[e, :, start : start + CHUNK] * jnp.exp2(old - top)

    def held(item):
        return m_s[item[1], :, item[0] : item[0] + CHUNK]

    marks = []
    first = 0
    for step, count in zip(NEIGHBOURS, pieces(rows, groups)):
        marks.append((first * 8, count * 8, there(step, sizes)[0].astype(F32)))
        first += count
    total = first * 8
    sides = 2 * rows * 8

    def halo_keys(begin, end, size):
        for start in range(begin, end, size):
            raw = halo_ref[start // 8 : (start + size) // 8].astype(F32).reshape(size, width)
            h = rms(raw, g0).astype(BF)
            spot = lax.broadcasted_iota(jnp.int32, (1, size), 1) + start
            ok = jnp.zeros((1, size), F32)
            for at, count, flag in marks:
                if at < start + size and at + count > start:
                    ok = jnp.where((spot >= at) & (spot < at + count), flag, ok)
            keep(h, tokens + start, ok)

    attend(0, tokens, 256, 2, lambda item: None, put)
    arrive(copies[:2])
    halo_keys(0, sides, 128)
    attend(tokens, sides, 384, 3, held, lambda item, top, acc: put(item, top, join(item, top, acc)))
    arrive(copies[2:])
    halo_keys(sides, total, 256)

    def tail(start, ctx):
        x = take(start)
        x = x + jnp.dot(ctx, wo_ref[...], preferred_element_type=F32)
        h = rms(x, g1).astype(BF)
        u = jax.nn.gelu(jnp.dot(h, wu_ref[...], preferred_element_type=F32)).astype(BF)
        x = x + jnp.dot(u, wd_ref[...], preferred_element_type=F32)
        f = rms(x, fg)
        for n, (r, g) in enumerate(spots[start // 8 : start // 8 + lot]):
            piece = f[n * 8 : n * 8 + 8]
            out_ref[r, g] = piece.astype(BF)
            for side, where in ((0, 0), (1, groups - 1)):
                if g == where:
                    for half in range(width // 128):
                        f_s[side, half, r * 8 : r * 8 + 8, :] = piece[:, half * 128 : half * 128 + 128]

    slots = [col_h.at[0], col_h.at[1], row_h.at[0], row_h.at[1]] + [cor_h.at[n] for n in range(4)]
    sources = [
        left_s, right_s, out_ref.at[0], out_ref.at[rows - 1],
        left_s.at[pl.ds(0, 8)], right_s.at[pl.ds(0, 8)],
        left_s.at[pl.ds(rows - 8, 8)], right_s.at[pl.ds(rows - 8, 8)],
    ]
    context = {}
    final = []

    def finals(item, top, acc):
        start, e = item
        acc = join(item, top, acc)
        context[e] = acc[0:head] / acc[head : head + 1]
        if e == HEADS - 1:
            ctx = jnp.concatenate([context[n] for n in range(HEADS)], axis=0)
            tail(start, ctx.T.astype(BF))
            if start == ready:
                for half in range(width // 128):
                    sl = slice(half * 128, half * 128 + 128)
                    left_s[:, sl] = f_s[0, half, pl.ds(0, rows, stride=8), :].astype(BF)
                    right_s[:, sl] = f_s[1, half, pl.ds(7, rows, stride=8), :].astype(BF)
                final.extend(swap(sizes, sources, slots, send2, recv2, None))

    attend(tokens + sides, total - sides, 256, 2, held, finals)
    leave(copies)
    arrive(final)
    leave(final)


def layer(sizes, field, gains, wq, wk, wv, wo, wu, wd, fg):
    rows, cols, width = field.shape
    groups = cols // 8
    tokens = rows * cols
    blocks = sum(pieces(rows, groups))
    keys = tokens + blocks * 8
    aug = width // HEADS + TAIL
    vm = pl.BlockSpec(memory_space=pltpu.VMEM)
    hbm = pl.BlockSpec(memory_space=pltpu.HBM)
    eight = pltpu.SemaphoreType.DMA((8,))
    field = field.reshape(rows, groups, 8, width)
    inputs = (field, gains, wq, wk, wv, wo, wu, wd, fg)
    inputs = tuple(pltpu.with_memory_space_constraint(a, pltpu.HBM) for a in inputs)
    final, row, col, corner = pl.pallas_call(
        functools.partial(layer_kernel, sizes),
        out_shape=(
            jax.ShapeDtypeStruct((rows, groups, 8, width), BF),
            jax.ShapeDtypeStruct((2, groups, 8, width), BF),
            jax.ShapeDtypeStruct((2, rows, width), BF),
            jax.ShapeDtypeStruct((4, 8, width), BF),
        ),
        in_specs=[hbm] * len(inputs),
        out_specs=(vm,) * 4,
        scratch_shapes=[pltpu.VMEM(a.shape, a.dtype) for a in inputs] + [
            pltpu.VMEM((blocks, 8, width), BF),
            pltpu.VMEM((width, tokens), BF),
            pltpu.VMEM((keys, width), BF),
            pltpu.VMEM((HEADS, aug, keys), BF),
            pltpu.VMEM((4, tokens, CHUNK), F32),
            pltpu.VMEM((HEADS, aug, tokens), F32),
            pltpu.VMEM((HEADS, 8, tokens), F32),
            pltpu.VMEM((2, width // 128, rows * 8, 128), F32),
            pltpu.VMEM((rows, width), BF),
            pltpu.VMEM((rows, width), BF),
            eight, eight, eight, eight,
            pltpu.SemaphoreType.DMA((len(inputs),)),
        ],
        compiler_params=pltpu.CompilerParams(
            collective_id=0, has_side_effects=True, vmem_limit_bytes=VMEM_LIMIT,
        ),
        name="layer",
    )(*inputs)
    return final.reshape(rows, cols, width), row.reshape(2, cols, width), col, corner


def conv_kernel(final_ref, row_h, col_h, cor_h, weight_ref, image_hbm, image_ref, fb_s, wp_s, up_s, sem):
    rows, cols, width = final_ref.shape
    tokens = rows * cols
    outs = weight_ref.shape[1]
    old = lax.broadcasted_iota(jnp.int32, (outs, outs), 0)
    new = lax.broadcasted_iota(jnp.int32, (outs, outs), 1)
    want = (new % (outs // SHUF)) * SHUF + new // (outs // SHUF)
    perm = jnp.where(old == want, 1.0, 0.0).astype(BF)
    for tap in range(9):
        sl = slice(tap * width, (tap + 1) * width)
        wp_s[sl, :] = jnp.dot(weight_ref[sl, :], perm, preferred_element_type=F32).astype(BF)
    col = lax.broadcasted_iota(jnp.int32, (1, cols, 1), 1)

    def spread(first, count, x, before, after):
        flat = x.reshape(count * cols, width)
        low = pltpu.roll(flat, 1, 0).reshape(count, cols, width)
        high = pltpu.roll(flat, count * cols - 1, 0).reshape(count, cols, width)
        fb_s[1, first : first + count] = x.astype(BF)
        fb_s[0, first : first + count] = jnp.where(col == 0, before, low).astype(BF)
        fb_s[2, first : first + count] = jnp.where(col == cols - 1, after, high).astype(BF)

    for r in range(0, rows, 8):
        before = col_h[0, r : r + 8, :].astype(F32)[:, None, :]
        after = col_h[1, r : r + 8, :].astype(F32)[:, None, :]
        spread(1 + r, 8, final_ref[r : r + 8].astype(F32), before, after)
    for side, at, pick in ((0, 0, 7), (1, rows + 1, 0)):
        before = cor_h[2 * side].astype(F32)[pick : pick + 1][:, None, :]
        after = cor_h[2 * side + 1].astype(F32)[pick : pick + 1][:, None, :]
        spread(at, 1, row_h[side].astype(F32)[None], before, after)

    step = 8
    quarter = outs // SHUF
    outs_going = []
    for r in range(0, rows, step):
        acc = jnp.zeros((step * cols, outs), F32)
        for a in range(3):
            for b in range(3):
                tap = a * 3 + b
                acc = acc + jnp.dot(
                    fb_s[b, r + a : r + a + step].reshape(step * cols, width),
                    wp_s[tap * width : (tap + 1) * width, :],
                    preferred_element_type=F32,
                )
        for k in range(step):
            part = acc[k * cols : (k + 1) * cols]
            slot = k % 2
            for j in range(SHUF):
                pair = j * quarter // 128
                up_s[slot, pl.ds(j, cols, stride=SHUF), :] = part[:, pair * 128 : pair * 128 + 128]
            t = up_s[slot].T
            lanes = lax.broadcasted_iota(jnp.int32, (1, cols * SHUF), 1)
            t = jnp.where(lanes % 2 == 0, t[:quarter], t[quarter : 2 * quarter])
            for c in range(quarter // SHUF):
                image_ref[c, (r + k) * SHUF : (r + k + 1) * SHUF, :] = t[c * SHUF : (c + 1) * SHUF]
        band = pl.ds(r * SHUF, step * SHUF)
        outs_going.append(pltpu.make_async_copy(
            image_ref.at[:, band], image_hbm.at[:, band], sem.at[r // step]
        ))
        outs_going[-1].start()
    for going in outs_going:
        going.wait()


def conv_image(final, row, col, corner, weight):
    rows, cols, width = final.shape
    outs = weight.shape[1]
    vm = pl.BlockSpec(memory_space=pltpu.VMEM)
    return pl.pallas_call(
        conv_kernel,
        out_shape=jax.ShapeDtypeStruct((outs // SHUF**2, rows * SHUF, cols * SHUF), F32),
        in_specs=[vm] * 5,
        out_specs=pl.BlockSpec(memory_space=pltpu.HBM),
        scratch_shapes=[
            pltpu.VMEM((outs // SHUF**2, rows * SHUF, cols * SHUF), F32),
            pltpu.VMEM((3, rows + 2, cols, width), BF),
            pltpu.VMEM(weight.shape, BF),
            pltpu.VMEM((2, cols * SHUF, 128), F32),
            pltpu.SemaphoreType.DMA((rows // 8,)),
        ],
        compiler_params=pltpu.CompilerParams(vmem_limit_bytes=VMEM_LIMIT),
        name="conv_image",
    )(final, row, col, corner, weight)


def local(sizes, field, gains, w_query, w_key, w_value, w_out, w_up, w_down, final_gain, conv_weight):
    final, row, col, corner = layer(
        sizes, field, gains[0], w_query[0], w_key[0], w_value[0], w_out[0], w_up[0], w_down[0],
        final_gain[None, :],
    )
    weight = conv_weight.reshape(-1, conv_weight.shape[3])
    return conv_image(final, row, col, corner, weight)


def solution(mesh):
    sizes = (mesh.shape["row"], mesh.shape["col"])
    return jax.shard_map(
        functools.partial(local, sizes),
        mesh=mesh,
        in_specs=(P("row", "col", None), P(), P(), P(), P(), P(), P(), P(), P(), P()),
        out_specs=P(None, "row", "col"),
        check_vma=False,
    )
```

```python
import functools

import jax
import jax.numpy as jnp
from jax import lax
from jax.experimental import pallas as pl
from jax.experimental.pallas import tpu as pltpu
from jax.sharding import PartitionSpec as P

HEADS = 8
HALO = 8
SHUF = 4
CHUNK = 256
TAIL = 16
LAG = 4
PACE = 2
OWN = 256
VMEM_LIMIT = 24 * 1024 * 1024
BF = jnp.bfloat16
F32 = jnp.float32
NEIGHBOURS = ((0, -1), (0, 1), (-1, 0), (-1, -1), (-1, 1), (1, 0), (1, -1), (1, 1))


def rms(values, gain):
    return values * lax.rsqrt(jnp.mean(values * values, axis=-1, keepdims=True) + 1e-06) * gain


def there(step, sizes):
    row, col = lax.axis_index("row"), lax.axis_index("col")
    nrow, ncol = row + step[0], col + step[1]
    ok = (nrow >= 0) & (nrow < sizes[0]) & (ncol >= 0) & (ncol < sizes[1])
    return ok, nrow, ncol


def greet(sizes):
    barrier = pltpu.get_barrier_semaphore()
    for step in NEIGHBOURS:
        ok, nrow, ncol = there(step, sizes)

        @pl.when(ok)
        def _():
            pl.semaphore_signal(
                barrier, inc=1, device_id=(nrow, ncol), device_id_type=pl.DeviceIdType.MESH
            )

    peers = jnp.int32(0)
    for step in NEIGHBOURS:
        peers = peers + there(step, sizes)[0].astype(jnp.int32)
    pl.semaphore_wait(barrier, peers)


def swap(sizes, sources, slots, send, recv, fills):
    copies = []
    for n, step in enumerate(NEIGHBOURS):
        ok, nrow, ncol = there(step, sizes)
        back = NEIGHBOURS.index((-step[0], -step[1]))
        copy = pltpu.make_async_remote_copy(
            src_ref=sources[n],
            dst_ref=slots[back],
            send_sem=send.at[n],
            recv_sem=recv.at[back],
            device_id=(nrow, ncol),
            device_id_type=pl.DeviceIdType.MESH,
        )
        arrival = pltpu.make_async_remote_copy(
            src_ref=slots[n],
            dst_ref=slots[n],
            send_sem=send.at[n],
            recv_sem=recv.at[n],
            device_id=(nrow, ncol),
            device_id_type=pl.DeviceIdType.MESH,
        )
        copies.append((ok, copy, arrival))
        if fills is not None:
            pl.when(jnp.logical_not(ok))(fills[n])
    for n in sorted(range(len(copies)), key=lambda n: -NEIGHBOURS[n][0]):
        pl.when(copies[n][0])(copies[n][1].start)
    return copies


def arrive(copies):
    for ok, _, arrival in copies:
        pl.when(ok)(arrival.wait_recv)


def leave(copies):
    for ok, copy, _ in copies:
        pl.when(ok)(copy.wait_send)


def pieces(rows, groups):
    return [rows] * 2 + [HALO * groups, HALO, HALO] * 2


def halo_start(sizes, field_ref, halo_ref, send, recv):
    rows, groups = field_ref.shape[:2]
    sources, slots, fills = [], [], []
    first = 0
    for step, count in zip(NEIGHBOURS, pieces(rows, groups)):
        dr, dc = step
        rsel = slice(0, rows) if dr == 0 else (slice(0, HALO) if dr < 0 else slice(rows - HALO, rows))
        slot = halo_ref.at[pl.ds(first, count)]
        if dc == 0:
            sources.append(field_ref.at[rsel])
            slots.append(slot.reshape(HALO, groups, 8, field_ref.shape[3]))
        else:
            sources.append(field_ref.at[rsel, 0 if dc < 0 else groups - 1])
            slots.append(slot)

        def fill(first=first, count=count):
            for k in range(0, count, HALO):
                halo_ref[first + k : first + k + HALO] = field_ref[0:HALO, 0]

        fills.append(fill)
        first += count
    return swap(sizes, sources, slots, send, recv, fills)


def nt_dot(left, right):
    return lax.dot_general(left, right, (((1,), (1,)), ((), ())), preferred_element_type=F32)


def layer_kernel(
    sizes,
    field_hbm, gains_hbm, wq_hbm, wk_hbm, wv_hbm, wo_hbm, wu_hbm, wd_hbm, fg_hbm,
    out_ref, row_h, col_h, cor_h,
    field_ref, gains_ref, wq_ref, wk_ref, wv_ref, wo_ref, wu_ref, wd_ref, fg_ref,
    halo_ref, qt_s, k_s, va_s, s_s, o_s, m_s, f_s, left_s, right_s,
    send, recv, send2, recv2, wsem,
):
    rows, groups = field_ref.shape[:2]
    width, tokens = qt_s.shape
    head = width // HEADS
    per = 128 // head
    loads = [
        pltpu.make_async_copy(src, dst, wsem.at[n])
        for n, (src, dst) in enumerate((
            (field_hbm, field_ref), (gains_hbm, gains_ref), (wq_hbm, wq_ref), (wk_hbm, wk_ref),
            (wv_hbm, wv_ref), (wo_hbm, wo_ref), (wu_hbm, wu_ref), (wd_hbm, wd_ref),
            (fg_hbm, fg_ref),
        ))
    ]
    for load in loads:
        load.start()
    for slot in (row_h, col_h, cor_h):
        slot[...] = jnp.zeros(slot.shape, BF)
    greet(sizes)
    loads[0].wait()
    copies = halo_start(sizes, field_ref, halo_ref, send, recv)
    for load in loads[1:]:
        load.wait()

    g0 = gains_ref[0:1, :]
    g1 = gains_ref[1:2, :]
    fg = fg_ref[...]
    wqt = wq_ref[...].T
    wvt = wv_ref[...].T

    def edge(spot):
        return spot[0] in (0, rows - 1) or spot[1] in (0, groups - 1)

    spots = [(r, g) for r in range(rows) for g in range(groups)]
    spots = [spot for spot in spots if edge(spot)] + [spot for spot in spots if not edge(spot)]
    lot = CHUNK // 8
    edges = sum(edge(spot) for spot in spots)
    starts = list(range(0, tokens, CHUNK))
    ready = max(start for start in starts if start < edges * 8)

    def take(start):
        part = spots[start // 8 : start // 8 + lot]
        return jnp.concatenate([field_ref[r, g].astype(F32) for r, g in part], axis=0)

    def keep(h, start, ok):
        count = h.shape[0]
        keys = slice(start, start + count)
        k_s[keys, :] = jnp.dot(h, wk_ref[...], preferred_element_type=F32).astype(BF)
        v = nt_dot(wvt, h)
        one = jnp.ones((TAIL, count), F32)
        if ok is not None:
            v = v * ok
            one = one * ok
        v = v.astype(BF)
        one = one.astype(BF)
        for e in range(HEADS):
            va_s[e, 0:head, keys] = v[e * head : (e + 1) * head]
            va_s[e, head : head + TAIL, keys] = one

    scale = head**-0.5 * 1.4426950408889634
    for start in starts:
        h = rms(take(start), g0).astype(BF)
        qt_s[:, start : start + CHUNK] = (nt_dot(wqt, h) * scale).astype(BF)
        keep(h, start, None)

    def scores(item, slot, first, count, step, base):
        start, e = item
        half, sub = e // per, e % per
        zero = jnp.zeros((head, CHUNK), BF)
        q = qt_s[e * head : (e + 1) * head, start : start + CHUNK]
        q = jnp.concatenate([q if n == sub else zero for n in range(per)], axis=0)
        top = base
        for kc in range(0, count, step):
            s = jnp.dot(
                k_s[first + kc : first + kc + step, half * 128 : half * 128 + 128], q,
                preferred_element_type=F32,
            )
            s_s[slot, kc : kc + step, :] = s
            part = jnp.max(s.reshape(step // 8, 8, CHUNK), axis=0)
            top = part if top is None else jnp.maximum(top, part)
            yield None
        yield jnp.max(top, axis=0, keepdims=True)

    def values(item, slot, first, count, step, top):
        start, e = item
        acc = None
        for kc in range(0, count, step):
            p = jnp.exp2((s_s[slot, kc : kc + step, :] - top).astype(BF))
            o = jnp.dot(
                va_s[e, :, first + kc : first + kc + step], p, preferred_element_type=F32
            )
            acc = o if acc is None else acc + o
            yield None
        yield acc

    items = [(start, e) for start in starts for e in range(HEADS)]

    def put(item, top, acc):
        start, e = item
        o_s[e, :, start : start + CHUNK] = acc
        m_s[e, :, start : start + CHUNK] = jnp.broadcast_to(top, (8, CHUNK))

    def join(item, top, acc):
        start, e = item
        old = m_s[e, 0:1, start : start + CHUNK]
        return acc + o_s[e, :, start : start + CHUNK] * jnp.exp2(old - top)

    def held(item):
        return m_s[item[1], :, item[0] : item[0] + CHUNK]

    marks = []
    first = 0
    for step, count in zip(NEIGHBOURS, pieces(rows, groups)):
        marks.append((first * 8, count * 8, there(step, sizes)[0].astype(F32)))
        first += count
    total = first * 8
    sides = 2 * rows * 8

    def halo_keys(begin, end, size):
        for start in range(begin, end, size):
            raw = halo_ref[start // 8 : (start + size) // 8].astype(F32).reshape(size, width)
            h = rms(raw, g0).astype(BF)
            spot = lax.broadcasted_iota(jnp.int32, (1, size), 1) + start
            ok = jnp.zeros((1, size), F32)
            for at, count, flag in marks:
                if at < start + size and at + count > start:
                    ok = jnp.where((spot >= at) & (spot < at + count), flag, ok)
            keep(h, tokens + start, ok)

    upper = sides + (total - sides) // 2
    wide = upper - sides

    def put_join(item, top, acc):
        put(item, top, join(item, top, acc))

    def enter(phase):
        arrive(copies[: 2] if phase == 1 else copies[2:5] if phase == 2 else copies[5:])
        halo_keys(*((0, sides), (sides, upper), (upper, total))[phase - 1], 128)

    def tail(start, ctx, low, high):
        lo, hi = low // 8, high // 8
        x = take(start)[low:high]
        x = x + jnp.dot(ctx[low:high], wo_ref[...], preferred_element_type=F32)
        yield
        h = rms(x, g1).astype(BF)
        yield
        wide_ff = wu_ref.shape[1]
        ups = None
        for at in list(range(0, wide_ff, width)) + [None]:
            last = ups
            if at is not None:
                ups = at, jnp.dot(h, wu_ref[:, at : at + width], preferred_element_type=F32)
            if last is not None:
                u = jax.nn.gelu(last[1]).astype(BF)
                x = x + jnp.dot(
                    u, wd_ref[last[0] : last[0] + width, :], preferred_element_type=F32
                )
            yield
        f = rms(x, fg)
        for n, (r, g) in enumerate(spots[start // 8 + lo : start // 8 + hi]):
            piece = f[n * 8 : n * 8 + 8]
            out_ref[r, g] = piece.astype(BF)
            for side, where in ((0, 0), (1, groups - 1)):
                if g == where:
                    for half in range(width // 128):
                        f_s[side, half, r * 8 : r * 8 + 8, :] = piece[:, half * 128 : half * 128 + 128]
        if start == ready and high == CHUNK:
            for half in range(width // 128):
                sl = slice(half * 128, half * 128 + 128)
                left_s[:, sl] = f_s[0, half, pl.ds(0, rows, stride=8), :].astype(BF)
                right_s[:, sl] = f_s[1, half, pl.ds(7, rows, stride=8), :].astype(BF)
            final.extend(swap(sizes, sources, slots, send2, recv2, None))

    slots = [
        col_h.at[0], col_h.at[1],
        row_h.at[0], cor_h.at[0], cor_h.at[1],
        row_h.at[1], cor_h.at[2], cor_h.at[3],
    ]
    sources = [
        left_s, right_s,
        out_ref.at[0], left_s.at[pl.ds(0, 8)], right_s.at[pl.ds(0, 8)],
        out_ref.at[rows - 1], left_s.at[pl.ds(rows - 8, 8)], right_s.at[pl.ds(rows - 8, 8)],
    ]
    context = {}
    final = []

    pending = []

    def finals(item, top, acc):
        start, e = item
        acc = join(item, top, acc)
        context[e] = acc[0:head] / acc[head : head + 1]
        if e == HEADS - 1:
            ctx = jnp.concatenate([context[n] for n in range(HEADS)], axis=0)
            ctx = ctx.T.astype(BF)
            if start == starts[-1]:
                part = CHUNK // 2
                pending.extend(tail(start, ctx, low, low + part) for low in range(0, CHUNK, part))
            else:
                pending.append(tail(start, ctx, 0, CHUNK))

    def advance():
        for going in list(pending):
            if next(going, pending) is pending:
                pending.remove(going)

    phases = [
        (0, tokens, OWN, put), (tokens, sides, sides, put_join),
        (tokens + sides, wide, wide, put_join), (tokens + upper, wide, wide, finals),
    ]
    work = [(n, item) for n in range(len(phases)) for item in items]
    tops = {}
    for n in range(len(work) + LAG):
        now = then = top = acc = None
        rounds = 0
        if n < len(work):
            phase, item = work[n]
            first, count, step, _ = phases[phase]
            if phase and item == items[0]:
                enter(phase)
            now = scores(item, n % (LAG + 1), first, count, step, held(item) if phase else None)
            rounds = count // step + 1
        if n >= LAG:
            phase, item = work[n - LAG]
            first, count, step, done = phases[phase]
            old = tops.pop(n - LAG)
            then = values(item, (n - LAG) % (LAG + 1), first, count, step, old)
            rounds = max(rounds, count // step + 1)
        for _ in range(rounds):
            top = top if now is None else next(now, top)
            acc = acc if then is None else next(then, acc)
        tops[n] = top
        if then is not None:
            done(item, old, acc)
        for _ in range(PACE):
            advance()
    while pending:
        advance()
    leave(copies)
    arrive(final)
    leave(final)


def layer(sizes, field, gains, wq, wk, wv, wo, wu, wd, fg):
    rows, cols, width = field.shape
    groups = cols // 8
    tokens = rows * cols
    blocks = sum(pieces(rows, groups))
    keys = tokens + blocks * 8
    aug = width // HEADS + TAIL
    vm = pl.BlockSpec(memory_space=pltpu.VMEM)
    hbm = pl.BlockSpec(memory_space=pltpu.HBM)
    eight = pltpu.SemaphoreType.DMA((8,))
    field = field.reshape(rows, groups, 8, width)
    inputs = (field, gains, wq, wk, wv, wo, wu, wd, fg)
    inputs = tuple(pltpu.with_memory_space_constraint(a, pltpu.HBM) for a in inputs)
    final, row, col, corner = pl.pallas_call(
        functools.partial(layer_kernel, sizes),
        out_shape=(
            jax.ShapeDtypeStruct((rows, groups, 8, width), BF),
            jax.ShapeDtypeStruct((2, groups, 8, width), BF),
            jax.ShapeDtypeStruct((2, rows, width), BF),
            jax.ShapeDtypeStruct((4, 8, width), BF),
        ),
        in_specs=[hbm] * len(inputs),
        out_specs=(vm,) * 4,
        scratch_shapes=[pltpu.VMEM(a.shape, a.dtype) for a in inputs] + [
            pltpu.VMEM((blocks, 8, width), BF),
            pltpu.VMEM((width, tokens), BF),
            pltpu.VMEM((keys, width), BF),
            pltpu.VMEM((HEADS, aug, keys), BF),
            pltpu.VMEM((LAG + 1, tokens, CHUNK), F32),
            pltpu.VMEM((HEADS, aug, tokens), F32),
            pltpu.VMEM((HEADS, 8, tokens), F32),
            pltpu.VMEM((2, width // 128, rows * 8, 128), F32),
            pltpu.VMEM((rows, width), BF),
            pltpu.VMEM((rows, width), BF),
            eight, eight, eight, eight,
            pltpu.SemaphoreType.DMA((len(inputs),)),
        ],
        compiler_params=pltpu.CompilerParams(
            collective_id=0, has_side_effects=True, vmem_limit_bytes=VMEM_LIMIT,
        ),
        name="layer",
    )(*inputs)
    return final.reshape(rows, cols, width), row.reshape(2, cols, width), col, corner


def conv_kernel(final_ref, row_h, col_h, cor_h, weight_ref, image_hbm, image_ref, fb_s, wp_s, up_s, sem):
    rows, cols, width = final_ref.shape
    tokens = rows * cols
    outs = weight_ref.shape[1]
    old = lax.broadcasted_iota(jnp.int32, (outs, outs), 0)
    new = lax.broadcasted_iota(jnp.int32, (outs, outs), 1)
    want = (new % (outs // SHUF)) * SHUF + new // (outs // SHUF)
    perm = jnp.where(old == want, 1.0, 0.0).astype(BF)
    for tap in range(9):
        sl = slice(tap * width, (tap + 1) * width)
        wp_s[sl, :] = jnp.dot(weight_ref[sl, :], perm, preferred_element_type=F32).astype(BF)
    col = lax.broadcasted_iota(jnp.int32, (1, cols, 1), 1)

    def spread(first, count, x, before, after):
        flat = x.reshape(count * cols, width)
        low = pltpu.roll(flat, 1, 0).reshape(count, cols, width)
        high = pltpu.roll(flat, count * cols - 1, 0).reshape(count, cols, width)
        fb_s[1, first : first + count] = x.astype(BF)
        fb_s[0, first : first + count] = jnp.where(col == 0, before, low).astype(BF)
        fb_s[2, first : first + count] = jnp.where(col == cols - 1, after, high).astype(BF)

    for r in range(0, rows, 8):
        before = col_h[0, r : r + 8, :].astype(F32)[:, None, :]
        after = col_h[1, r : r + 8, :].astype(F32)[:, None, :]
        spread(1 + r, 8, final_ref[r : r + 8].astype(F32), before, after)
    for side, at, pick in ((0, 0, 7), (1, rows + 1, 0)):
        before = cor_h[2 * side].astype(F32)[pick : pick + 1][:, None, :]
        after = cor_h[2 * side + 1].astype(F32)[pick : pick + 1][:, None, :]
        spread(at, 1, row_h[side].astype(F32)[None], before, after)

    step = 8
    quarter = outs // SHUF
    outs_going = []
    for r in range(0, rows, step):
        acc = jnp.zeros((step * cols, outs), F32)
        for a in range(3):
            for b in range(3):
                tap = a * 3 + b
                acc = acc + jnp.dot(
                    fb_s[b, r + a : r + a + step].reshape(step * cols, width),
                    wp_s[tap * width : (tap + 1) * width, :],
                    preferred_element_type=F32,
                )
        for k in range(step):
            part = acc[k * cols : (k + 1) * cols]
            slot = k % 2
            for j in range(SHUF):
                pair = j * quarter // 128
                up_s[slot, pl.ds(j, cols, stride=SHUF), :] = part[:, pair * 128 : pair * 128 + 128]
            t = up_s[slot].T
            lanes = lax.broadcasted_iota(jnp.int32, (1, cols * SHUF), 1)
            t = jnp.where(lanes % 2 == 0, t[:quarter], t[quarter : 2 * quarter])
            for c in range(quarter // SHUF):
                image_ref[c, (r + k) * SHUF : (r + k + 1) * SHUF, :] = t[c * SHUF : (c + 1) * SHUF]
        band = pl.ds(r * SHUF, step * SHUF)
        outs_going.append(pltpu.make_async_copy(
            image_ref.at[:, band], image_hbm.at[:, band], sem.at[r // step]
        ))
        outs_going[-1].start()
    for going in outs_going:
        going.wait()


def conv_image(final, row, col, corner, weight):
    rows, cols, width = final.shape
    outs = weight.shape[1]
    vm = pl.BlockSpec(memory_space=pltpu.VMEM)
    return pl.pallas_call(
        conv_kernel,
        out_shape=jax.ShapeDtypeStruct((outs // SHUF**2, rows * SHUF, cols * SHUF), F32),
        in_specs=[vm] * 5,
        out_specs=pl.BlockSpec(memory_space=pltpu.HBM),
        scratch_shapes=[
            pltpu.VMEM((outs // SHUF**2, rows * SHUF, cols * SHUF), F32),
            pltpu.VMEM((3, rows + 2, cols, width), BF),
            pltpu.VMEM(weight.shape, BF),
            pltpu.VMEM((2, cols * SHUF, 128), F32),
            pltpu.SemaphoreType.DMA((rows // 8,)),
        ],
        compiler_params=pltpu.CompilerParams(vmem_limit_bytes=VMEM_LIMIT),
        name="conv_image",
    )(final, row, col, corner, weight)


def local(sizes, field, gains, w_query, w_key, w_value, w_out, w_up, w_down, final_gain, conv_weight):
    final, row, col, corner = layer(
        sizes, field, gains[0], w_query[0], w_key[0], w_value[0], w_out[0], w_up[0], w_down[0],
        final_gain[None, :],
    )
    weight = conv_weight.reshape(-1, conv_weight.shape[3])
    return conv_image(final, row, col, corner, weight)


def solution(mesh):
    sizes = (mesh.shape["row"], mesh.shape["col"])
    return jax.shard_map(
        functools.partial(local, sizes),
        mesh=mesh,
        in_specs=(P("row", "col", None), P(), P(), P(), P(), P(), P(), P(), P(), P()),
        out_specs=P(None, "row", "col"),
        check_vma=False,
    )
```

```python
import functools

import jax
import jax.numpy as jnp
from jax import lax
from jax.experimental import pallas as pl
from jax.experimental.pallas import tpu as pltpu
from jax.sharding import PartitionSpec as P

HEADS = 8
HALO = 8
SHUF = 4
CHUNK = 256
TAIL = 16
LAG = 4
PACE = 3
OWN = 256
VMEM_LIMIT = 24 * 1024 * 1024
BF = jnp.bfloat16
F32 = jnp.float32
NEIGHBOURS = ((0, -1), (0, 1), (-1, 0), (-1, -1), (-1, 1), (1, 0), (1, -1), (1, 1))


def rms(values, gain):
    return values * lax.rsqrt(jnp.mean(values * values, axis=-1, keepdims=True) + 1e-06) * gain


def there(step, sizes):
    row, col = lax.axis_index("row"), lax.axis_index("col")
    nrow, ncol = row + step[0], col + step[1]
    ok = (nrow >= 0) & (nrow < sizes[0]) & (ncol >= 0) & (ncol < sizes[1])
    return ok, nrow, ncol


def greet(sizes):
    barrier = pltpu.get_barrier_semaphore()
    for step in NEIGHBOURS:
        ok, nrow, ncol = there(step, sizes)

        @pl.when(ok)
        def _():
            pl.semaphore_signal(
                barrier, inc=1, device_id=(nrow, ncol), device_id_type=pl.DeviceIdType.MESH
            )

    peers = jnp.int32(0)
    for step in NEIGHBOURS:
        peers = peers + there(step, sizes)[0].astype(jnp.int32)
    pl.semaphore_wait(barrier, peers)


def swap(sizes, sources, slots, send, recv, fills):
    copies = []
    for n, step in enumerate(NEIGHBOURS):
        ok, nrow, ncol = there(step, sizes)
        back = NEIGHBOURS.index((-step[0], -step[1]))
        copy = pltpu.make_async_remote_copy(
            src_ref=sources[n],
            dst_ref=slots[back],
            send_sem=send.at[n],
            recv_sem=recv.at[back],
            device_id=(nrow, ncol),
            device_id_type=pl.DeviceIdType.MESH,
        )
        arrival = pltpu.make_async_remote_copy(
            src_ref=slots[n],
            dst_ref=slots[n],
            send_sem=send.at[n],
            recv_sem=recv.at[n],
            device_id=(nrow, ncol),
            device_id_type=pl.DeviceIdType.MESH,
        )
        copies.append((ok, copy, arrival))
        if fills is not None:
            pl.when(jnp.logical_not(ok))(fills[n])
    for n in sorted(range(len(copies)), key=lambda n: -NEIGHBOURS[n][0]):
        pl.when(copies[n][0])(copies[n][1].start)
    return copies


def arrive(copies):
    for ok, _, arrival in copies:
        pl.when(ok)(arrival.wait_recv)


def leave(copies):
    for ok, copy, _ in copies:
        pl.when(ok)(copy.wait_send)


def pieces(rows, groups):
    return [rows] * 2 + [HALO * groups, HALO, HALO] * 2


def halo_start(sizes, field_ref, halo_ref, send, recv):
    rows, groups = field_ref.shape[:2]
    sources, slots, fills = [], [], []
    first = 0
    for step, count in zip(NEIGHBOURS, pieces(rows, groups)):
        dr, dc = step
        rsel = slice(0, rows) if dr == 0 else (slice(0, HALO) if dr < 0 else slice(rows - HALO, rows))
        slot = halo_ref.at[pl.ds(first, count)]
        if dc == 0:
            sources.append(field_ref.at[rsel])
            slots.append(slot.reshape(HALO, groups, 8, field_ref.shape[3]))
        else:
            sources.append(field_ref.at[rsel, 0 if dc < 0 else groups - 1])
            slots.append(slot)

        def fill(first=first, count=count):
            for k in range(0, count, HALO):
                halo_ref[first + k : first + k + HALO] = field_ref[0:HALO, 0]

        fills.append(fill)
        first += count
    return swap(sizes, sources, slots, send, recv, fills)


def nt_dot(left, right):
    return lax.dot_general(left, right, (((1,), (1,)), ((), ())), preferred_element_type=F32)


def layer_kernel(
    sizes,
    field_hbm, gains_hbm, wq_hbm, wk_hbm, wv_hbm, wo_hbm, wu_hbm, wd_hbm, fg_hbm,
    out_ref, row_h, col_h, cor_h,
    field_ref, gains_ref, wq_ref, wk_ref, wv_ref, wo_ref, wu_ref, wd_ref, fg_ref,
    halo_ref, qt_s, k_s, va_s, s_s, o_s, m_s, f_s, left_s, right_s,
    send, recv, send2, recv2, wsem,
):
    rows, groups = field_ref.shape[:2]
    width, tokens = qt_s.shape
    head = width // HEADS
    per = 128 // head
    loads = [
        pltpu.make_async_copy(src, dst, wsem.at[n])
        for n, (src, dst) in enumerate((
            (field_hbm, field_ref), (gains_hbm, gains_ref), (wq_hbm, wq_ref), (wk_hbm, wk_ref),
            (wv_hbm, wv_ref), (wo_hbm, wo_ref), (wu_hbm, wu_ref), (wd_hbm, wd_ref),
            (fg_hbm, fg_ref),
        ))
    ]
    for load in loads:
        load.start()
    for slot in (row_h, col_h, cor_h):
        slot[...] = jnp.zeros(slot.shape, BF)
    greet(sizes)
    loads[0].wait()
    copies = halo_start(sizes, field_ref, halo_ref, send, recv)
    for load in loads[1:5] + loads[8:]:
        load.wait()

    g0 = gains_ref[0:1, :]
    g1 = gains_ref[1:2, :]
    fg = fg_ref[...]
    wqt = wq_ref[...].T
    wvt = wv_ref[...].T

    def edge(spot):
        return spot[0] in (0, rows - 1) or spot[1] in (0, groups - 1)

    spots = [(r, g) for r in range(rows) for g in range(groups)]
    spots = [spot for spot in spots if edge(spot)] + [spot for spot in spots if not edge(spot)]
    lot = CHUNK // 8
    edges = sum(edge(spot) for spot in spots)
    starts = list(range(0, tokens, CHUNK))
    ready = max(start for start in starts if start < edges * 8)

    def take(start):
        part = spots[start // 8 : start // 8 + lot]
        return jnp.concatenate([field_ref[r, g].astype(F32) for r, g in part], axis=0)

    def keep(h, start, ok):
        count = h.shape[0]
        keys = slice(start, start + count)
        k_s[keys, :] = jnp.dot(h, wk_ref[...], preferred_element_type=F32).astype(BF)
        v = nt_dot(wvt, h)
        one = jnp.ones((TAIL, count), F32)
        if ok is not None:
            v = v * ok
            one = one * ok
        v = v.astype(BF)
        one = one.astype(BF)
        for e in range(HEADS):
            va_s[e, 0:head, keys] = v[e * head : (e + 1) * head]
            va_s[e, head : head + TAIL, keys] = one

    scale = head**-0.5 * 1.4426950408889634
    for start in starts:
        h = rms(take(start), g0).astype(BF)
        qt_s[:, start : start + CHUNK] = (nt_dot(wqt, h) * scale).astype(BF)
        keep(h, start, None)

    def scores(item, slot, first, count, step, base):
        start, e = item
        half, sub = e // per, e % per
        zero = jnp.zeros((head, CHUNK), BF)
        q = qt_s[e * head : (e + 1) * head, start : start + CHUNK]
        q = jnp.concatenate([q if n == sub else zero for n in range(per)], axis=0)
        top = base
        for kc in range(0, count, step):
            s = jnp.dot(
                k_s[first + kc : first + kc + step, half * 128 : half * 128 + 128], q,
                preferred_element_type=F32,
            )
            s_s[slot, kc : kc + step, :] = s
            part = jnp.max(s.reshape(step // 8, 8, CHUNK), axis=0)
            top = part if top is None else jnp.maximum(top, part)
            yield None
        yield jnp.max(top, axis=0, keepdims=True)

    def values(item, slot, first, count, step, top):
        start, e = item
        acc = None
        for kc in range(0, count, step):
            p = jnp.exp2((s_s[slot, kc : kc + step, :] - top).astype(BF))
            o = jnp.dot(
                va_s[e, :, first + kc : first + kc + step], p, preferred_element_type=F32
            )
            acc = o if acc is None else acc + o
            yield None
        yield acc

    items = [(start, e) for start in starts for e in range(HEADS)]

    def put(item, top, acc):
        start, e = item
        o_s[e, :, start : start + CHUNK] = acc
        m_s[e, :, start : start + CHUNK] = jnp.broadcast_to(top, (8, CHUNK))

    def join(item, top, acc):
        start, e = item
        old = m_s[e, 0:1, start : start + CHUNK]
        return acc + o_s[e, :, start : start + CHUNK] * jnp.exp2(old - top)

    def held(item):
        return m_s[item[1], :, item[0] : item[0] + CHUNK]

    marks = []
    first = 0
    for step, count in zip(NEIGHBOURS, pieces(rows, groups)):
        marks.append((first * 8, count * 8, there(step, sizes)[0].astype(F32)))
        first += count
    total = first * 8
    sides = 2 * rows * 8

    def halo_keys(begin, end, size):
        for start in range(begin, end, size):
            raw = halo_ref[start // 8 : (start + size) // 8].astype(F32).reshape(size, width)
            h = rms(raw, g0).astype(BF)
            spot = lax.broadcasted_iota(jnp.int32, (1, size), 1) + start
            ok = jnp.zeros((1, size), F32)
            for at, count, flag in marks:
                if at < start + size and at + count > start:
                    ok = jnp.where((spot >= at) & (spot < at + count), flag, ok)
            keep(h, tokens + start, ok)

    upper = sides + (total - sides) // 2
    wide = upper - sides

    def put_join(item, top, acc):
        put(item, top, join(item, top, acc))

    def enter(phase):
        arrive(copies[: 2] if phase == 1 else copies[2:5] if phase == 2 else copies[5:])
        halo_keys(*((0, sides), (sides, upper), (upper, total))[phase - 1], 128)
        if phase == 3:
            for load in loads[5:8]:
                load.wait()

    def tail(start, ctx, low, high):
        lo, hi = low // 8, high // 8
        x = take(start)[low:high]
        x = x + jnp.dot(ctx[low:high], wo_ref[...], preferred_element_type=F32)
        yield
        h = rms(x, g1).astype(BF)
        yield
        wide_ff = wu_ref.shape[1]
        ups = None
        for at in list(range(0, wide_ff, width)) + [None]:
            last = ups
            if at is not None:
                ups = at, jnp.dot(h, wu_ref[:, at : at + width], preferred_element_type=F32)
            if last is not None:
                u = jax.nn.gelu(last[1]).astype(BF)
                x = x + jnp.dot(
                    u, wd_ref[last[0] : last[0] + width, :], preferred_element_type=F32
                )
            yield
        f = rms(x, fg)
        for n, (r, g) in enumerate(spots[start // 8 + lo : start // 8 + hi]):
            piece = f[n * 8 : n * 8 + 8]
            out_ref[r, g] = piece.astype(BF)
            for side, where in ((0, 0), (1, groups - 1)):
                if g == where:
                    for half in range(width // 128):
                        f_s[side, half, r * 8 : r * 8 + 8, :] = piece[:, half * 128 : half * 128 + 128]
        if start == ready and high == CHUNK:
            for half in range(width // 128):
                sl = slice(half * 128, half * 128 + 128)
                left_s[:, sl] = f_s[0, half, pl.ds(0, rows, stride=8), :].astype(BF)
                right_s[:, sl] = f_s[1, half, pl.ds(7, rows, stride=8), :].astype(BF)
            final.extend(swap(sizes, sources, slots, send2, recv2, None))

    slots = [
        col_h.at[0], col_h.at[1],
        row_h.at[0], cor_h.at[0], cor_h.at[1],
        row_h.at[1], cor_h.at[2], cor_h.at[3],
    ]
    sources = [
        left_s, right_s,
        out_ref.at[0], left_s.at[pl.ds(0, 8)], right_s.at[pl.ds(0, 8)],
        out_ref.at[rows - 1], left_s.at[pl.ds(rows - 8, 8)], right_s.at[pl.ds(rows - 8, 8)],
    ]
    context = {}
    final = []

    pending = []

    def finals(item, top, acc):
        start, e = item
        acc = join(item, top, acc)
        context[e] = acc[0:head] / acc[head : head + 1]
        if e == HEADS - 1:
            ctx = jnp.concatenate([context[n] for n in range(HEADS)], axis=0)
            ctx = ctx.T.astype(BF)
            if start == starts[-1]:
                part = CHUNK // 2
                pending.extend(tail(start, ctx, low, low + part) for low in range(0, CHUNK, part))
            else:
                pending.append(tail(start, ctx, 0, CHUNK))

    def advance():
        for going in list(pending):
            if next(going, pending) is pending:
                pending.remove(going)

    phases = [
        (0, tokens, OWN, put), (tokens, sides, sides, put_join),
        (tokens + sides, wide, wide, put_join), (tokens + upper, wide, wide, finals),
    ]
    early = [item for item in items if item[0] <= ready]
    late = [item for item in items if item[0] > ready]
    work = [(0, item) for item in items]
    work += [(n, item) for part in (early, late) for n in range(1, len(phases)) for item in part]
    tops = {}
    for n in range(len(work) + LAG):
        now = then = top = acc = None
        rounds = 0
        if n < len(work):
            phase, item = work[n]
            first, count, step, _ = phases[phase]
            if phase and item == early[0]:
                enter(phase)
            now = scores(item, n % (LAG + 1), first, count, step, held(item) if phase else None)
            rounds = count // step + 1
        if n >= LAG:
            phase, item = work[n - LAG]
            first, count, step, done = phases[phase]
            old = tops.pop(n - LAG)
            then = values(item, (n - LAG) % (LAG + 1), first, count, step, old)
            rounds = max(rounds, count // step + 1)
        for _ in range(rounds):
            top = top if now is None else next(now, top)
            acc = acc if then is None else next(then, acc)
        tops[n] = top
        if then is not None:
            done(item, old, acc)
        for _ in range(PACE):
            advance()
    while pending:
        advance()
    leave(copies)
    arrive(final)
    leave(final)


def layer(sizes, field, gains, wq, wk, wv, wo, wu, wd, fg):
    rows, cols, width = field.shape
    groups = cols // 8
    tokens = rows * cols
    blocks = sum(pieces(rows, groups))
    keys = tokens + blocks * 8
    aug = width // HEADS + TAIL
    vm = pl.BlockSpec(memory_space=pltpu.VMEM)
    hbm = pl.BlockSpec(memory_space=pltpu.HBM)
    eight = pltpu.SemaphoreType.DMA((8,))
    field = field.reshape(rows, groups, 8, width)
    inputs = (field, gains, wq, wk, wv, wo, wu, wd, fg)
    inputs = tuple(pltpu.with_memory_space_constraint(a, pltpu.HBM) for a in inputs)
    final, row, col, corner = pl.pallas_call(
        functools.partial(layer_kernel, sizes),
        out_shape=(
            jax.ShapeDtypeStruct((rows, groups, 8, width), BF),
            jax.ShapeDtypeStruct((2, groups, 8, width), BF),
            jax.ShapeDtypeStruct((2, rows, width), BF),
            jax.ShapeDtypeStruct((4, 8, width), BF),
        ),
        in_specs=[hbm] * len(inputs),
        out_specs=(vm,) * 4,
        scratch_shapes=[pltpu.VMEM(a.shape, a.dtype) for a in inputs] + [
            pltpu.VMEM((blocks, 8, width), BF),
            pltpu.VMEM((width, tokens), BF),
            pltpu.VMEM((keys, width), BF),
            pltpu.VMEM((HEADS, aug, keys), BF),
            pltpu.VMEM((LAG + 1, tokens, CHUNK), F32),
            pltpu.VMEM((HEADS, aug, tokens), F32),
            pltpu.VMEM((HEADS, 8, tokens), F32),
            pltpu.VMEM((2, width // 128, rows * 8, 128), F32),
            pltpu.VMEM((rows, width), BF),
            pltpu.VMEM((rows, width), BF),
            eight, eight, eight, eight,
            pltpu.SemaphoreType.DMA((len(inputs),)),
        ],
        compiler_params=pltpu.CompilerParams(
            collective_id=0, has_side_effects=True, vmem_limit_bytes=VMEM_LIMIT,
        ),
        name="layer",
    )(*inputs)
    return final.reshape(rows, cols, width), row.reshape(2, cols, width), col, corner


def conv_kernel(final_ref, row_h, col_h, cor_h, weight_ref, image_hbm, image_ref, fb_s, wp_s, up_s, sem):
    rows, cols, width = final_ref.shape
    tokens = rows * cols
    outs = weight_ref.shape[1]
    old = lax.broadcasted_iota(jnp.int32, (outs, outs), 0)
    new = lax.broadcasted_iota(jnp.int32, (outs, outs), 1)
    want = (new % (outs // SHUF)) * SHUF + new // (outs // SHUF)
    perm = jnp.where(old == want, 1.0, 0.0).astype(BF)
    for tap in range(9):
        sl = slice(tap * width, (tap + 1) * width)
        wp_s[sl, :] = jnp.dot(weight_ref[sl, :], perm, preferred_element_type=F32).astype(BF)
    col = lax.broadcasted_iota(jnp.int32, (1, cols, 1), 1)

    def spread(first, count, x, before, after):
        flat = x.reshape(count * cols, width)
        low = pltpu.roll(flat, 1, 0).reshape(count, cols, width)
        high = pltpu.roll(flat, count * cols - 1, 0).reshape(count, cols, width)
        fb_s[1, first : first + count] = x.astype(BF)
        fb_s[0, first : first + count] = jnp.where(col == 0, before, low).astype(BF)
        fb_s[2, first : first + count] = jnp.where(col == cols - 1, after, high).astype(BF)

    for r in range(0, rows, 8):
        before = col_h[0, r : r + 8, :].astype(F32)[:, None, :]
        after = col_h[1, r : r + 8, :].astype(F32)[:, None, :]
        spread(1 + r, 8, final_ref[r : r + 8].astype(F32), before, after)
    for side, at, pick in ((0, 0, 7), (1, rows + 1, 0)):
        before = cor_h[2 * side].astype(F32)[pick : pick + 1][:, None, :]
        after = cor_h[2 * side + 1].astype(F32)[pick : pick + 1][:, None, :]
        spread(at, 1, row_h[side].astype(F32)[None], before, after)

    step = 8
    quarter = outs // SHUF
    outs_going = []
    for r in range(0, rows, step):
        acc = jnp.zeros((step * cols, outs), F32)
        for a in range(3):
            for b in range(3):
                tap = a * 3 + b
                acc = acc + jnp.dot(
                    fb_s[b, r + a : r + a + step].reshape(step * cols, width),
                    wp_s[tap * width : (tap + 1) * width, :],
                    preferred_element_type=F32,
                )
        for k in range(step):
            part = acc[k * cols : (k + 1) * cols]
            slot = k % 2
            for j in range(SHUF):
                pair = j * quarter // 128
                up_s[slot, pl.ds(j, cols, stride=SHUF), :] = part[:, pair * 128 : pair * 128 + 128]
            t = up_s[slot].T
            lanes = lax.broadcasted_iota(jnp.int32, (1, cols * SHUF), 1)
            t = jnp.where(lanes % 2 == 0, t[:quarter], t[quarter : 2 * quarter])
            for c in range(quarter // SHUF):
                image_ref[c, (r + k) * SHUF : (r + k + 1) * SHUF, :] = t[c * SHUF : (c + 1) * SHUF]
        band = pl.ds(r * SHUF, step * SHUF)
        outs_going.append(pltpu.make_async_copy(
            image_ref.at[:, band], image_hbm.at[:, band], sem.at[r // step]
        ))
        outs_going[-1].start()
    for going in outs_going:
        going.wait()


def conv_image(final, row, col, corner, weight):
    rows, cols, width = final.shape
    outs = weight.shape[1]
    vm = pl.BlockSpec(memory_space=pltpu.VMEM)
    return pl.pallas_call(
        conv_kernel,
        out_shape=jax.ShapeDtypeStruct((outs // SHUF**2, rows * SHUF, cols * SHUF), F32),
        in_specs=[vm] * 5,
        out_specs=pl.BlockSpec(memory_space=pltpu.HBM),
        scratch_shapes=[
            pltpu.VMEM((outs // SHUF**2, rows * SHUF, cols * SHUF), F32),
            pltpu.VMEM((3, rows + 2, cols, width), BF),
            pltpu.VMEM(weight.shape, BF),
            pltpu.VMEM((2, cols * SHUF, 128), F32),
            pltpu.SemaphoreType.DMA((rows // 8,)),
        ],
        compiler_params=pltpu.CompilerParams(vmem_limit_bytes=VMEM_LIMIT),
        name="conv_image",
    )(final, row, col, corner, weight)


def local(sizes, field, gains, w_query, w_key, w_value, w_out, w_up, w_down, final_gain, conv_weight):
    final, row, col, corner = layer(
        sizes, field, gains[0], w_query[0], w_key[0], w_value[0], w_out[0], w_up[0], w_down[0],
        final_gain[None, :],
    )
    weight = conv_weight.reshape(-1, conv_weight.shape[3])
    return conv_image(final, row, col, corner, weight)


def solution(mesh):
    sizes = (mesh.shape["row"], mesh.shape["col"])
    return jax.shard_map(
        functools.partial(local, sizes),
        mesh=mesh,
        in_specs=(P("row", "col", None), P(), P(), P(), P(), P(), P(), P(), P(), P()),
        out_specs=P(None, "row", "col"),
        check_vma=False,
    )
```

```python
import functools

import jax
import jax.numpy as jnp
from jax import lax
from jax.experimental import pallas as pl
from jax.experimental.pallas import tpu as pltpu
from jax.sharding import PartitionSpec as P

HEADS = 8
HALO = 8
SHUF = 4
CHUNK = 256
TAIL = 16
LAG = 4
PACE = 3
OWN = 256
VMEM_LIMIT = 24 * 1024 * 1024
BF = jnp.bfloat16
F32 = jnp.float32
NEIGHBOURS = ((0, -1), (0, 1), (-1, 0), (1, 0), (-1, -1), (-1, 1), (1, -1), (1, 1))


def rms(values, gain):
    return values * lax.rsqrt(jnp.mean(values * values, axis=-1, keepdims=True) + 1e-06) * gain


def there(step, sizes):
    row, col = lax.axis_index("row"), lax.axis_index("col")
    nrow, ncol = row + step[0], col + step[1]
    ok = (nrow >= 0) & (nrow < sizes[0]) & (ncol >= 0) & (ncol < sizes[1])
    return ok, nrow, ncol


def greet(sizes):
    barrier = pltpu.get_barrier_semaphore()
    for step in NEIGHBOURS:
        ok, nrow, ncol = there(step, sizes)

        @pl.when(ok)
        def _():
            pl.semaphore_signal(
                barrier, inc=1, device_id=(nrow, ncol), device_id_type=pl.DeviceIdType.MESH
            )

    peers = jnp.int32(0)
    for step in NEIGHBOURS:
        peers = peers + there(step, sizes)[0].astype(jnp.int32)
    pl.semaphore_wait(barrier, peers)


def swap(sizes, sources, slots, send, recv, fills, count):
    copies = []
    for n, step in enumerate(NEIGHBOURS):
        ok, nrow, ncol = there(step, sizes)
        back = NEIGHBOURS.index((-step[0], -step[1]))
        copy = pltpu.make_async_remote_copy(
            src_ref=sources[n],
            dst_ref=slots[back],
            send_sem=send.at[n],
            recv_sem=recv.at[back],
            device_id=(nrow, ncol),
            device_id_type=pl.DeviceIdType.MESH,
        )
        arrival = pltpu.make_async_remote_copy(
            src_ref=slots[n],
            dst_ref=slots[n],
            send_sem=send.at[n],
            recv_sem=recv.at[n],
            device_id=(nrow, ncol),
            device_id_type=pl.DeviceIdType.MESH,
        )
        if n < count:
            copies.append((ok, copy, arrival))
        if fills is not None:
            pl.when(jnp.logical_not(ok))(fills[n])
    for ok, copy, _ in reversed(copies):
        pl.when(ok)(copy.start)
    return copies


def relay(sizes, slots, groups, send, recv):
    copies = []
    for n, (dr, dc) in enumerate(NEIGHBOURS):
        if dr == 0 or dc == 0:
            continue
        held = slots[NEIGHBOURS.index((dr, 0))].at[:, 0 if dc > 0 else groups - 1]
        ok = there((dr, -dc), sizes)[0]
        _, nrow, ncol = there((0, -dc), sizes)
        copy, arrival = (
            pltpu.make_async_remote_copy(
                src_ref=src,
                dst_ref=slots[n],
                send_sem=send.at[n],
                recv_sem=recv.at[n],
                device_id=(nrow, ncol),
                device_id_type=pl.DeviceIdType.MESH,
            )
            for src in (held, slots[n])
        )
        pl.when(ok)(copy.start)
        copies.append((ok, copy, there((dr, dc), sizes)[0], arrival))
    return copies


def arrive(copies):
    for ok, _, arrival in copies:
        pl.when(ok)(arrival.wait_recv)


def leave(copies):
    for ok, copy, _ in copies:
        pl.when(ok)(copy.wait_send)


def pieces(rows, groups):
    return [rows] * 2 + [HALO * groups] * 2 + [HALO] * 4


def halo_start(sizes, field_ref, halo_ref, send, recv):
    rows, groups = field_ref.shape[:2]
    sources, slots, fills = [], [], []
    first = 0
    for step, count in zip(NEIGHBOURS, pieces(rows, groups)):
        dr, dc = step
        rsel = slice(0, rows) if dr == 0 else (slice(0, HALO) if dr < 0 else slice(rows - HALO, rows))
        slot = halo_ref.at[pl.ds(first, count)]
        if dc == 0:
            sources.append(field_ref.at[rsel])
            slots.append(slot.reshape(HALO, groups, 8, field_ref.shape[3]))
        else:
            sources.append(field_ref.at[rsel, 0 if dc < 0 else groups - 1])
            slots.append(slot)

        def fill(first=first, count=count):
            for k in range(0, count, HALO):
                halo_ref[first + k : first + k + HALO] = field_ref[0:HALO, 0]

        fills.append(fill)
        first += count
    return swap(sizes, sources, slots, send, recv, fills, 4), slots


def nt_dot(left, right):
    return lax.dot_general(left, right, (((1,), (1,)), ((), ())), preferred_element_type=F32)


def layer_kernel(
    sizes,
    field_hbm, gains_hbm, wq_hbm, wk_hbm, wv_hbm, wo_hbm, wu_hbm, wd_hbm, fg_hbm,
    out_ref, row_h, col_h, cor_h,
    field_ref, gains_ref, wq_ref, wk_ref, wv_ref, wo_ref, wu_ref, wd_ref, fg_ref,
    halo_ref, qt_s, k_s, va_s, s_s, o_s, m_s, f_s, left_s, right_s,
    send, recv, send2, recv2, wsem,
):
    rows, groups = field_ref.shape[:2]
    width, tokens = qt_s.shape
    head = width // HEADS
    per = 128 // head
    loads = [
        pltpu.make_async_copy(src, dst, wsem.at[n])
        for n, (src, dst) in enumerate((
            (field_hbm, field_ref), (gains_hbm, gains_ref), (wq_hbm, wq_ref), (wk_hbm, wk_ref),
            (wv_hbm, wv_ref), (wo_hbm, wo_ref), (wu_hbm, wu_ref), (wd_hbm, wd_ref),
            (fg_hbm, fg_ref),
        ))
    ]
    for load in loads:
        load.start()
    for slot in (row_h, col_h, cor_h):
        slot[...] = jnp.zeros(slot.shape, BF)
    greet(sizes)
    loads[0].wait()
    copies, landed = halo_start(sizes, field_ref, halo_ref, send, recv)
    for load in loads[1:5] + loads[8:]:
        load.wait()

    g0 = gains_ref[0:1, :]
    g1 = gains_ref[1:2, :]
    fg = fg_ref[...]
    wqt = wq_ref[...].T
    wvt = wv_ref[...].T

    def edge(spot):
        return spot[0] in (0, rows - 1) or spot[1] in (0, groups - 1)

    spots = [(r, g) for r in range(rows) for g in range(groups)]
    spots = [spot for spot in spots if edge(spot)] + [spot for spot in spots if not edge(spot)]
    lot = CHUNK // 8
    edges = sum(edge(spot) for spot in spots)
    starts = list(range(0, tokens, CHUNK))
    ready = max(start for start in starts if start < edges * 8)

    def take(start):
        part = spots[start // 8 : start // 8 + lot]
        return jnp.concatenate([field_ref[r, g].astype(F32) for r, g in part], axis=0)

    def keep(h, start, ok):
        count = h.shape[0]
        keys = slice(start, start + count)
        k_s[keys, :] = jnp.dot(h, wk_ref[...], preferred_element_type=F32).astype(BF)
        v = nt_dot(wvt, h)
        one = jnp.ones((TAIL, count), F32)
        if ok is not None:
            v = v * ok
            one = one * ok
        v = v.astype(BF)
        one = one.astype(BF)
        for e in range(HEADS):
            va_s[e, 0:head, keys] = v[e * head : (e + 1) * head]
            va_s[e, head : head + TAIL, keys] = one

    scale = head**-0.5 * 1.4426950408889634
    for start in starts:
        h = rms(take(start), g0).astype(BF)
        qt_s[:, start : start + CHUNK] = (nt_dot(wqt, h) * scale).astype(BF)
        keep(h, start, None)

    def scores(item, slot, first, count, step, base):
        start, e = item
        half, sub = e // per, e % per
        zero = jnp.zeros((head, CHUNK), BF)
        q = qt_s[e * head : (e + 1) * head, start : start + CHUNK]
        q = jnp.concatenate([q if n == sub else zero for n in range(per)], axis=0)
        top = base
        for kc in range(0, count, step):
            s = jnp.dot(
                k_s[first + kc : first + kc + step, half * 128 : half * 128 + 128], q,
                preferred_element_type=F32,
            )
            s_s[slot, kc : kc + step, :] = s
            part = jnp.max(s.reshape(step // 8, 8, CHUNK), axis=0)
            top = part if top is None else jnp.maximum(top, part)
            yield None
        yield jnp.max(top, axis=0, keepdims=True)

    def values(item, slot, first, count, step, top):
        start, e = item
        acc = None
        for kc in range(0, count, step):
            p = jnp.exp2((s_s[slot, kc : kc + step, :] - top).astype(BF))
            o = jnp.dot(
                va_s[e, :, first + kc : first + kc + step], p, preferred_element_type=F32
            )
            acc = o if acc is None else acc + o
            yield None
        yield acc

    items = [(start, e) for start in starts for e in range(HEADS)]

    def put(item, top, acc):
        start, e = item
        o_s[e, :, start : start + CHUNK] = acc
        m_s[e, :, start : start + CHUNK] = jnp.broadcast_to(top, (8, CHUNK))

    def join(item, top, acc):
        start, e = item
        old = m_s[e, 0:1, start : start + CHUNK]
        return acc + o_s[e, :, start : start + CHUNK] * jnp.exp2(old - top)

    def held(item):
        return m_s[item[1], :, item[0] : item[0] + CHUNK]

    marks = []
    first = 0
    for step, count in zip(NEIGHBOURS, pieces(rows, groups)):
        marks.append((first * 8, count * 8, there(step, sizes)[0].astype(F32)))
        first += count
    total = first * 8
    sides = 2 * rows * 8

    def halo_keys(begin, end, size):
        for start in range(begin, end, size):
            raw = halo_ref[start // 8 : (start + size) // 8].astype(F32).reshape(size, width)
            h = rms(raw, g0).astype(BF)
            spot = lax.broadcasted_iota(jnp.int32, (1, size), 1) + start
            ok = jnp.zeros((1, size), F32)
            for at, count, flag in marks:
                if at < start + size and at + count > start:
                    ok = jnp.where((spot >= at) & (spot < at + count), flag, ok)
            keep(h, tokens + start, ok)

    upper = sides + 2 * HALO * groups * 8
    passed = []

    def put_join(item, top, acc):
        put(item, top, join(item, top, acc))

    def enter(phase):
        if phase < 3:
            arrive(copies[2 * phase - 2 : 2 * phase])
        if phase == 2:
            passed.extend(relay(sizes, landed, groups, send, recv))
        if phase == 3:
            for _, _, ok, arrival in passed:
                pl.when(ok)(arrival.wait_recv)
        halo_keys(*((0, sides), (sides, upper), (upper, total))[phase - 1], 128)
        if phase == 3:
            for load in loads[5:8]:
                load.wait()

    def tail(start, ctx, low, high):
        lo, hi = low // 8, high // 8
        x = take(start)[low:high]
        x = x + jnp.dot(ctx[low:high], wo_ref[...], preferred_element_type=F32)
        yield
        h = rms(x, g1).astype(BF)
        yield
        wide_ff = wu_ref.shape[1]
        ups = None
        for at in list(range(0, wide_ff, width)) + [None]:
            last = ups
            if at is not None:
                ups = at, jnp.dot(h, wu_ref[:, at : at + width], preferred_element_type=F32)
            if last is not None:
                u = jax.nn.gelu(last[1]).astype(BF)
                x = x + jnp.dot(
                    u, wd_ref[last[0] : last[0] + width, :], preferred_element_type=F32
                )
            yield
        f = rms(x, fg)
        for n, (r, g) in enumerate(spots[start // 8 + lo : start // 8 + hi]):
            piece = f[n * 8 : n * 8 + 8]
            out_ref[r, g] = piece.astype(BF)
            for side, where in ((0, 0), (1, groups - 1)):
                if g == where:
                    for half in range(width // 128):
                        f_s[side, half, r * 8 : r * 8 + 8, :] = piece[:, half * 128 : half * 128 + 128]
        if start == ready and high == CHUNK:
            for half in range(width // 128):
                sl = slice(half * 128, half * 128 + 128)
                left_s[:, sl] = f_s[0, half, pl.ds(0, rows, stride=8), :].astype(BF)
                right_s[:, sl] = f_s[1, half, pl.ds(7, rows, stride=8), :].astype(BF)
            final.extend(swap(sizes, sources, slots, send2, recv2, None, 8))

    slots = [col_h.at[0], col_h.at[1], row_h.at[0], row_h.at[1]] + [cor_h.at[n] for n in range(4)]
    sources = [
        left_s, right_s, out_ref.at[0], out_ref.at[rows - 1],
        left_s.at[pl.ds(0, 8)], right_s.at[pl.ds(0, 8)],
        left_s.at[pl.ds(rows - 8, 8)], right_s.at[pl.ds(rows - 8, 8)],
    ]
    context = {}
    final = []

    pending = []

    def finals(item, top, acc):
        start, e = item
        acc = join(item, top, acc)
        context[e] = acc[0:head] / acc[head : head + 1]
        if e == HEADS - 1:
            ctx = jnp.concatenate([context[n] for n in range(HEADS)], axis=0)
            ctx = ctx.T.astype(BF)
            if start == starts[-1]:
                part = CHUNK // 2
                pending.extend(tail(start, ctx, low, low + part) for low in range(0, CHUNK, part))
            else:
                pending.append(tail(start, ctx, 0, CHUNK))

    def advance():
        for going in list(pending):
            if next(going, pending) is pending:
                pending.remove(going)

    phases = [
        (0, tokens, OWN, put), (tokens, sides, sides, put_join),
        (tokens + sides, upper - sides, upper - sides, put_join),
        (tokens + upper, total - upper, total - upper, finals),
    ]
    early = [item for item in items if item[0] <= ready]
    late = [item for item in items if item[0] > ready]
    work = [(0, item) for item in items]
    work += [(n, item) for n in (1, 2) for item in items]
    work += [(3, item) for item in early + late]
    tops = {}
    for n in range(len(work) + LAG):
        now = then = top = acc = None
        rounds = 0
        if n < len(work):
            phase, item = work[n]
            first, count, step, _ = phases[phase]
            if phase and item == early[0]:
                enter(phase)
            now = scores(item, n % (LAG + 1), first, count, step, held(item) if phase else None)
            rounds = count // step + 1
        if n >= LAG:
            phase, item = work[n - LAG]
            first, count, step, done = phases[phase]
            old = tops.pop(n - LAG)
            then = values(item, (n - LAG) % (LAG + 1), first, count, step, old)
            rounds = max(rounds, count // step + 1)
        for _ in range(rounds):
            top = top if now is None else next(now, top)
            acc = acc if then is None else next(then, acc)
        tops[n] = top
        if then is not None:
            done(item, old, acc)
        for _ in range(PACE):
            advance()
    while pending:
        advance()
    leave(copies)
    for ok, copy, _, _ in passed:
        pl.when(ok)(copy.wait_send)
    arrive(final)
    leave(final)


def layer(sizes, field, gains, wq, wk, wv, wo, wu, wd, fg):
    rows, cols, width = field.shape
    groups = cols // 8
    tokens = rows * cols
    blocks = sum(pieces(rows, groups))
    keys = tokens + blocks * 8
    aug = width // HEADS + TAIL
    vm = pl.BlockSpec(memory_space=pltpu.VMEM)
    hbm = pl.BlockSpec(memory_space=pltpu.HBM)
    eight = pltpu.SemaphoreType.DMA((8,))
    field = field.reshape(rows, groups, 8, width)
    inputs = (field, gains, wq, wk, wv, wo, wu, wd, fg)
    inputs = tuple(pltpu.with_memory_space_constraint(a, pltpu.HBM) for a in inputs)
    final, row, col, corner = pl.pallas_call(
        functools.partial(layer_kernel, sizes),
        out_shape=(
            jax.ShapeDtypeStruct((rows, groups, 8, width), BF),
            jax.ShapeDtypeStruct((2, groups, 8, width), BF),
            jax.ShapeDtypeStruct((2, rows, width), BF),
            jax.ShapeDtypeStruct((4, 8, width), BF),
        ),
        in_specs=[hbm] * len(inputs),
        out_specs=(vm,) * 4,
        scratch_shapes=[pltpu.VMEM(a.shape, a.dtype) for a in inputs] + [
            pltpu.VMEM((blocks, 8, width), BF),
            pltpu.VMEM((width, tokens), BF),
            pltpu.VMEM((keys, width), BF),
            pltpu.VMEM((HEADS, aug, keys), BF),
            pltpu.VMEM((LAG + 1, tokens, CHUNK), F32),
            pltpu.VMEM((HEADS, aug, tokens), F32),
            pltpu.VMEM((HEADS, 8, tokens), F32),
            pltpu.VMEM((2, width // 128, rows * 8, 128), F32),
            pltpu.VMEM((rows, width), BF),
            pltpu.VMEM((rows, width), BF),
            eight, eight, eight, eight,
            pltpu.SemaphoreType.DMA((len(inputs),)),
        ],
        compiler_params=pltpu.CompilerParams(
            collective_id=0, has_side_effects=True, vmem_limit_bytes=VMEM_LIMIT,
        ),
        name="layer",
    )(*inputs)
    return final.reshape(rows, cols, width), row.reshape(2, cols, width), col, corner


def conv_kernel(final_ref, row_h, col_h, cor_h, weight_ref, image_hbm, image_ref, fb_s, wp_s, up_s, sem):
    rows, cols, width = final_ref.shape
    tokens = rows * cols
    outs = weight_ref.shape[1]
    old = lax.broadcasted_iota(jnp.int32, (outs, outs), 0)
    new = lax.broadcasted_iota(jnp.int32, (outs, outs), 1)
    want = (new % (outs // SHUF)) * SHUF + new // (outs // SHUF)
    perm = jnp.where(old == want, 1.0, 0.0).astype(BF)
    for tap in range(9):
        sl = slice(tap * width, (tap + 1) * width)
        wp_s[sl, :] = jnp.dot(weight_ref[sl, :], perm, preferred_element_type=F32).astype(BF)
    col = lax.broadcasted_iota(jnp.int32, (1, cols, 1), 1)

    def spread(first, count, x, before, after):
        flat = x.reshape(count * cols, width)
        low = pltpu.roll(flat, 1, 0).reshape(count, cols, width)
        high = pltpu.roll(flat, count * cols - 1, 0).reshape(count, cols, width)
        fb_s[1, first : first + count] = x.astype(BF)
        fb_s[0, first : first + count] = jnp.where(col == 0, before, low).astype(BF)
        fb_s[2, first : first + count] = jnp.where(col == cols - 1, after, high).astype(BF)

    for r in range(0, rows, 8):
        before = col_h[0, r : r + 8, :].astype(F32)[:, None, :]
        after = col_h[1, r : r + 8, :].astype(F32)[:, None, :]
        spread(1 + r, 8, final_ref[r : r + 8].astype(F32), before, after)
    for side, at, pick in ((0, 0, 7), (1, rows + 1, 0)):
        before = cor_h[2 * side].astype(F32)[pick : pick + 1][:, None, :]
        after = cor_h[2 * side + 1].astype(F32)[pick : pick + 1][:, None, :]
        spread(at, 1, row_h[side].astype(F32)[None], before, after)

    step = 8
    quarter = outs // SHUF
    outs_going = []
    for r in range(0, rows, step):
        acc = jnp.zeros((step * cols, outs), F32)
        for a in range(3):
            for b in range(3):
                tap = a * 3 + b
                acc = acc + jnp.dot(
                    fb_s[b, r + a : r + a + step].reshape(step * cols, width),
                    wp_s[tap * width : (tap + 1) * width, :],
                    preferred_element_type=F32,
                )
        for k in range(step):
            part = acc[k * cols : (k + 1) * cols]
            slot = k % 2
            for j in range(SHUF):
                pair = j * quarter // 128
                up_s[slot, pl.ds(j, cols, stride=SHUF), :] = part[:, pair * 128 : pair * 128 + 128]
            t = up_s[slot].T
            lanes = lax.broadcasted_iota(jnp.int32, (1, cols * SHUF), 1)
            t = jnp.where(lanes % 2 == 0, t[:quarter], t[quarter : 2 * quarter])
            for c in range(quarter // SHUF):
                image_ref[c, (r + k) * SHUF : (r + k + 1) * SHUF, :] = t[c * SHUF : (c + 1) * SHUF]
        band = pl.ds(r * SHUF, step * SHUF)
        outs_going.append(pltpu.make_async_copy(
            image_ref.at[:, band], image_hbm.at[:, band], sem.at[r // step]
        ))
        outs_going[-1].start()
    for going in outs_going:
        going.wait()


def conv_image(final, row, col, corner, weight):
    rows, cols, width = final.shape
    outs = weight.shape[1]
    vm = pl.BlockSpec(memory_space=pltpu.VMEM)
    return pl.pallas_call(
        conv_kernel,
        out_shape=jax.ShapeDtypeStruct((outs // SHUF**2, rows * SHUF, cols * SHUF), F32),
        in_specs=[vm] * 5,
        out_specs=pl.BlockSpec(memory_space=pltpu.HBM),
        scratch_shapes=[
            pltpu.VMEM((outs // SHUF**2, rows * SHUF, cols * SHUF), F32),
            pltpu.VMEM((3, rows + 2, cols, width), BF),
            pltpu.VMEM(weight.shape, BF),
            pltpu.VMEM((2, cols * SHUF, 128), F32),
            pltpu.SemaphoreType.DMA((rows // 8,)),
        ],
        compiler_params=pltpu.CompilerParams(vmem_limit_bytes=VMEM_LIMIT),
        name="conv_image",
    )(final, row, col, corner, weight)


def local(sizes, field, gains, w_query, w_key, w_value, w_out, w_up, w_down, final_gain, conv_weight):
    final, row, col, corner = layer(
        sizes, field, gains[0], w_query[0], w_key[0], w_value[0], w_out[0], w_up[0], w_down[0],
        final_gain[None, :],
    )
    weight = conv_weight.reshape(-1, conv_weight.shape[3])
    return conv_image(final, row, col, corner, weight)


def solution(mesh):
    sizes = (mesh.shape["row"], mesh.shape["col"])
    return jax.shard_map(
        functools.partial(local, sizes),
        mesh=mesh,
        in_specs=(P("row", "col", None), P(), P(), P(), P(), P(), P(), P(), P(), P()),
        out_specs=P(None, "row", "col"),
        check_vma=False,
    )
```

```python
import functools

import jax
import jax.numpy as jnp
from jax import lax
from jax.experimental import pallas as pl
from jax.experimental.pallas import tpu as pltpu
from jax.sharding import PartitionSpec as P

HEADS = 8
HALO = 8
SHUF = 4
CHUNK = 256
TAIL = 16
LAG = 4
PACE = 3
OWN = 256
VMEM_LIMIT = 24 * 1024 * 1024
BF = jnp.bfloat16
F32 = jnp.float32
NEIGHBOURS = ((0, -1), (0, 1), (-1, 0), (1, 0), (-1, -1), (-1, 1), (1, -1), (1, 1))


def rms(values, gain):
    return values * lax.rsqrt(jnp.mean(values * values, axis=-1, keepdims=True) + 1e-06) * gain


def there(step, sizes):
    row, col = lax.axis_index("row"), lax.axis_index("col")
    nrow, ncol = row + step[0], col + step[1]
    ok = (nrow >= 0) & (nrow < sizes[0]) & (ncol >= 0) & (ncol < sizes[1])
    return ok, nrow, ncol


def greet(sizes):
    barrier = pltpu.get_barrier_semaphore()
    for step in NEIGHBOURS:
        ok, nrow, ncol = there(step, sizes)

        @pl.when(ok)
        def _():
            pl.semaphore_signal(
                barrier, inc=1, device_id=(nrow, ncol), device_id_type=pl.DeviceIdType.MESH
            )

    peers = jnp.int32(0)
    for step in NEIGHBOURS:
        peers = peers + there(step, sizes)[0].astype(jnp.int32)
    pl.semaphore_wait(barrier, peers)


def swap(sizes, sources, slots, send, recv, fills, count):
    copies = []
    for n, step in enumerate(NEIGHBOURS):
        ok, nrow, ncol = there(step, sizes)
        back = NEIGHBOURS.index((-step[0], -step[1]))
        copy = pltpu.make_async_remote_copy(
            src_ref=sources[n],
            dst_ref=slots[back],
            send_sem=send.at[n],
            recv_sem=recv.at[back],
            device_id=(nrow, ncol),
            device_id_type=pl.DeviceIdType.MESH,
        )
        arrival = pltpu.make_async_remote_copy(
            src_ref=slots[n],
            dst_ref=slots[n],
            send_sem=send.at[n],
            recv_sem=recv.at[n],
            device_id=(nrow, ncol),
            device_id_type=pl.DeviceIdType.MESH,
        )
        if n < count:
            copies.append((ok, copy, arrival))
        if fills is not None:
            pl.when(jnp.logical_not(ok))(fills[n])
    for ok, copy, _ in reversed(copies):
        pl.when(ok)(copy.start)
    return copies


def relay(sizes, slots, groups, send, recv):
    copies = []
    for n, (dr, dc) in enumerate(NEIGHBOURS):
        if dr == 0 or dc == 0:
            continue
        held = slots[NEIGHBOURS.index((dr, 0))].at[:, 0 if dc > 0 else groups - 1]
        ok = there((dr, -dc), sizes)[0]
        _, nrow, ncol = there((0, -dc), sizes)
        copy, arrival = (
            pltpu.make_async_remote_copy(
                src_ref=src,
                dst_ref=slots[n],
                send_sem=send.at[n],
                recv_sem=recv.at[n],
                device_id=(nrow, ncol),
                device_id_type=pl.DeviceIdType.MESH,
            )
            for src in (held, slots[n])
        )
        pl.when(ok)(copy.start)
        copies.append((ok, copy, there((dr, dc), sizes)[0], arrival))
    return copies


def arrive(copies):
    for ok, _, arrival in copies:
        pl.when(ok)(arrival.wait_recv)


def leave(copies):
    for ok, copy, _ in copies:
        pl.when(ok)(copy.wait_send)


def pieces(rows, groups):
    return [rows] * 2 + [HALO * groups] * 2 + [HALO] * 4


def halo_start(sizes, field_ref, halo_ref, send, recv):
    rows, groups = field_ref.shape[:2]
    sources, slots, fills = [], [], []
    first = 0
    for step, count in zip(NEIGHBOURS, pieces(rows, groups)):
        dr, dc = step
        rsel = slice(0, rows) if dr == 0 else (slice(0, HALO) if dr < 0 else slice(rows - HALO, rows))
        slot = halo_ref.at[pl.ds(first, count)]
        if dc == 0:
            sources.append(field_ref.at[rsel])
            slots.append(slot.reshape(HALO, groups, 8, field_ref.shape[3]))
        else:
            sources.append(field_ref.at[rsel, 0 if dc < 0 else groups - 1])
            slots.append(slot)

        def fill(first=first, count=count):
            for k in range(0, count, HALO):
                halo_ref[first + k : first + k + HALO] = field_ref[0:HALO, 0]

        fills.append(fill)
        first += count
    return swap(sizes, sources, slots, send, recv, fills, 4), slots


def nt_dot(left, right):
    return lax.dot_general(left, right, (((1,), (1,)), ((), ())), preferred_element_type=F32)


def layer_kernel(
    sizes,
    field_hbm, gains_hbm, wq_hbm, wk_hbm, wv_hbm, wo_hbm, wu_hbm, wd_hbm, fg_hbm,
    out_ref, row_h, col_h, cor_h,
    field_ref, gains_ref, wq_ref, wk_ref, wv_ref, wo_ref, wu_ref, wd_ref, fg_ref,
    halo_ref, qt_s, k_s, va_s, s_s, o_s, m_s, f_s, left_s, right_s,
    send, recv, send2, recv2, wsem,
):
    rows, groups = field_ref.shape[:2]
    width, tokens = qt_s.shape
    head = width // HEADS
    per = 128 // head
    loads = [
        pltpu.make_async_copy(src, dst, wsem.at[n])
        for n, (src, dst) in enumerate((
            (field_hbm, field_ref), (gains_hbm, gains_ref), (wq_hbm, wq_ref), (wk_hbm, wk_ref),
            (wv_hbm, wv_ref), (wo_hbm, wo_ref), (wu_hbm, wu_ref), (wd_hbm, wd_ref),
            (fg_hbm, fg_ref),
        ))
    ]
    for load in loads:
        load.start()
    for slot in (row_h, col_h, cor_h):
        slot[...] = jnp.zeros(slot.shape, BF)
    greet(sizes)
    loads[0].wait()
    copies, landed = halo_start(sizes, field_ref, halo_ref, send, recv)
    for load in loads[1:5] + loads[8:]:
        load.wait()

    g0 = gains_ref[0:1, :]
    g1 = gains_ref[1:2, :]
    fg = fg_ref[...]
    wqt = wq_ref[...].T
    wvt = wv_ref[...].T

    def edge(spot):
        return spot[0] in (0, rows - 1) or spot[1] in (0, groups - 1)

    spots = [(r, g) for r in range(rows) for g in range(groups)]
    spots = [spot for spot in spots if edge(spot)] + [spot for spot in spots if not edge(spot)]
    lot = CHUNK // 8
    edges = sum(edge(spot) for spot in spots)
    starts = list(range(0, tokens, CHUNK))
    ready = max(start for start in starts if start < edges * 8)

    def take(start):
        part = spots[start // 8 : start // 8 + lot]
        return jnp.concatenate([field_ref[r, g].astype(F32) for r, g in part], axis=0)

    def keep(h, start, ok):
        count = h.shape[0]
        keys = slice(start, start + count)
        k_s[keys, :] = jnp.dot(h, wk_ref[...], preferred_element_type=F32).astype(BF)
        v = nt_dot(wvt, h)
        one = jnp.ones((TAIL, count), F32)
        if ok is not None:
            v = v * ok
            one = one * ok
        v = v.astype(BF)
        one = one.astype(BF)
        for e in range(HEADS):
            va_s[e, 0:head, keys] = v[e * head : (e + 1) * head]
            va_s[e, head : head + TAIL, keys] = one

    scale = head**-0.5 * 1.4426950408889634
    for start in starts:
        h = rms(take(start), g0).astype(BF)
        qt_s[:, start : start + CHUNK] = (nt_dot(wqt, h) * scale).astype(BF)
        keep(h, start, None)

    def scores(item, slot, first, count, step, base):
        start, e = item
        half, sub = e // per, e % per
        zero = jnp.zeros((head, CHUNK), BF)
        q = qt_s[e * head : (e + 1) * head, start : start + CHUNK]
        q = jnp.concatenate([q if n == sub else zero for n in range(per)], axis=0)
        top = base
        for kc in range(0, count, step):
            s = jnp.dot(
                k_s[first + kc : first + kc + step, half * 128 : half * 128 + 128], q,
                preferred_element_type=F32,
            )
            s_s[slot, kc : kc + step, :] = s
            part = jnp.max(s.reshape(step // 8, 8, CHUNK), axis=0)
            top = part if top is None else jnp.maximum(top, part)
            yield None
        yield jnp.max(top, axis=0, keepdims=True)

    def values(item, slot, first, count, step, top):
        start, e = item
        acc = None
        for kc in range(0, count, step):
            p = jnp.exp2((s_s[slot, kc : kc + step, :] - top).astype(BF))
            o = jnp.dot(
                va_s[e, :, first + kc : first + kc + step], p, preferred_element_type=F32
            )
            acc = o if acc is None else acc + o
            yield None
        yield acc

    items = [(start, e) for start in starts for e in range(HEADS)]

    def put(item, top, acc):
        start, e = item
        o_s[e, :, start : start + CHUNK] = acc
        m_s[e, :, start : start + CHUNK] = jnp.broadcast_to(top, (8, CHUNK))

    def join(item, top, acc):
        start, e = item
        old = m_s[e, 0:1, start : start + CHUNK]
        return acc + o_s[e, :, start : start + CHUNK] * jnp.exp2(old - top)

    def held(item):
        return m_s[item[1], :, item[0] : item[0] + CHUNK]

    marks = []
    first = 0
    for step, count in zip(NEIGHBOURS, pieces(rows, groups)):
        marks.append((first * 8, count * 8, there(step, sizes)[0].astype(F32)))
        first += count
    total = first * 8
    sides = 2 * rows * 8

    def halo_keys(begin, end, size):
        for start in range(begin, end, size):
            raw = halo_ref[start // 8 : (start + size) // 8].astype(F32).reshape(size, width)
            h = rms(raw, g0).astype(BF)
            spot = lax.broadcasted_iota(jnp.int32, (1, size), 1) + start
            ok = jnp.zeros((1, size), F32)
            for at, count, flag in marks:
                if at < start + size and at + count > start:
                    ok = jnp.where((spot >= at) & (spot < at + count), flag, ok)
            keep(h, tokens + start, ok)

    upper = sides + 2 * HALO * groups * 8
    passed = []

    def put_join(item, top, acc):
        put(item, top, join(item, top, acc))

    def enter(phase):
        if phase < 3:
            arrive(copies[2 * phase - 2 : 2 * phase])
        if phase == 2:
            passed.extend(relay(sizes, landed, groups, send, recv))
        if phase == 3:
            for _, _, ok, arrival in passed:
                pl.when(ok)(arrival.wait_recv)
        halo_keys(*((0, sides), (sides, upper), (upper, total))[phase - 1], 128)
        if phase == 3:
            for load in loads[5:8]:
                load.wait()

    def tail(start, ctx, low, high):
        lo, hi = low // 8, high // 8
        x = take(start)[low:high]
        x = x + jnp.dot(ctx[low:high], wo_ref[...], preferred_element_type=F32)
        yield
        h = rms(x, g1).astype(BF)
        yield
        wide_ff = wu_ref.shape[1]
        ups = None
        for at in list(range(0, wide_ff, width)) + [None]:
            last = ups
            if at is not None:
                ups = at, jnp.dot(h, wu_ref[:, at : at + width], preferred_element_type=F32)
            if last is not None:
                u = jax.nn.gelu(last[1]).astype(BF)
                x = x + jnp.dot(
                    u, wd_ref[last[0] : last[0] + width, :], preferred_element_type=F32
                )
            yield
        f = rms(x, fg)
        for n, (r, g) in enumerate(spots[start // 8 + lo : start // 8 + hi]):
            piece = f[n * 8 : n * 8 + 8]
            out_ref[r, g] = piece.astype(BF)
            for side, where in ((0, 0), (1, groups - 1)):
                if g == where:
                    for half in range(width // 128):
                        f_s[side, half, r * 8 : r * 8 + 8, :] = piece[:, half * 128 : half * 128 + 128]
        if start == ready and high == CHUNK:
            for half in range(width // 128):
                sl = slice(half * 128, half * 128 + 128)
                left_s[:, sl] = f_s[0, half, pl.ds(0, rows, stride=8), :].astype(BF)
                right_s[:, sl] = f_s[1, half, pl.ds(7, rows, stride=8), :].astype(BF)
            final.extend(swap(sizes, sources, slots, send2, recv2, None, 8))

    slots = [col_h.at[0], col_h.at[1], row_h.at[0], row_h.at[1]] + [cor_h.at[n] for n in range(4)]
    sources = [
        left_s, right_s, out_ref.at[0], out_ref.at[rows - 1],
        left_s.at[pl.ds(0, 8)], right_s.at[pl.ds(0, 8)],
        left_s.at[pl.ds(rows - 8, 8)], right_s.at[pl.ds(rows - 8, 8)],
    ]
    context = {}
    final = []

    pending = []

    def finals(item, top, acc):
        start, e = item
        acc = join(item, top, acc)
        context[e] = acc[0:head] / acc[head : head + 1]
        if e == HEADS - 1:
            ctx = jnp.concatenate([context[n] for n in range(HEADS)], axis=0)
            ctx = ctx.T.astype(BF)
            if start == starts[-1]:
                part = CHUNK // 2
                pending.extend(tail(start, ctx, low, low + part) for low in range(0, CHUNK, part))
            else:
                pending.append(tail(start, ctx, 0, CHUNK))

    def advance():
        for going in list(pending):
            if next(going, pending) is pending:
                pending.remove(going)

    phases = [
        (0, tokens, OWN, put), (tokens, sides, sides, put_join),
        (tokens + sides, upper - sides, upper - sides, put_join),
        (tokens + upper, total - upper, total - upper, finals),
    ]
    early = [item for item in items if item[0] <= ready]
    late = [item for item in items if item[0] > ready]
    work = [(0, item) for item in items]
    work += [(1, item) for item in items] + [(2, item) for item in early]
    work += [(3, item) for item in early]
    work += [(n, item) for n in (2, 3) for item in late]
    tops = {}
    for n in range(len(work) + LAG):
        now = then = top = acc = None
        rounds = 0
        if n < len(work):
            phase, item = work[n]
            first, count, step, _ = phases[phase]
            if phase and item == early[0]:
                enter(phase)
            now = scores(item, n % (LAG + 1), first, count, step, held(item) if phase else None)
            rounds = count // step + 1
        if n >= LAG:
            phase, item = work[n - LAG]
            first, count, step, done = phases[phase]
            old = tops.pop(n - LAG)
            then = values(item, (n - LAG) % (LAG + 1), first, count, step, old)
            rounds = max(rounds, count // step + 1)
        for _ in range(rounds):
            top = top if now is None else next(now, top)
            acc = acc if then is None else next(then, acc)
        tops[n] = top
        if then is not None:
            done(item, old, acc)
        for _ in range(PACE):
            advance()
    while pending:
        advance()
    leave(copies)
    for ok, copy, _, _ in passed:
        pl.when(ok)(copy.wait_send)
    arrive(final)
    leave(final)


def layer(sizes, field, gains, wq, wk, wv, wo, wu, wd, fg):
    rows, cols, width = field.shape
    groups = cols // 8
    tokens = rows * cols
    blocks = sum(pieces(rows, groups))
    keys = tokens + blocks * 8
    aug = width // HEADS + TAIL
    vm = pl.BlockSpec(memory_space=pltpu.VMEM)
    hbm = pl.BlockSpec(memory_space=pltpu.HBM)
    eight = pltpu.SemaphoreType.DMA((8,))
    field = field.reshape(rows, groups, 8, width)
    inputs = (field, gains, wq, wk, wv, wo, wu, wd, fg)
    inputs = tuple(pltpu.with_memory_space_constraint(a, pltpu.HBM) for a in inputs)
    final, row, col, corner = pl.pallas_call(
        functools.partial(layer_kernel, sizes),
        out_shape=(
            jax.ShapeDtypeStruct((rows, groups, 8, width), BF),
            jax.ShapeDtypeStruct((2, groups, 8, width), BF),
            jax.ShapeDtypeStruct((2, rows, width), BF),
            jax.ShapeDtypeStruct((4, 8, width), BF),
        ),
        in_specs=[hbm] * len(inputs),
        out_specs=(vm,) * 4,
        scratch_shapes=[pltpu.VMEM(a.shape, a.dtype) for a in inputs] + [
            pltpu.VMEM((blocks, 8, width), BF),
            pltpu.VMEM((width, tokens), BF),
            pltpu.VMEM((keys, width), BF),
            pltpu.VMEM((HEADS, aug, keys), BF),
            pltpu.VMEM((LAG + 1, tokens, CHUNK), F32),
            pltpu.VMEM((HEADS, aug, tokens), F32),
            pltpu.VMEM((HEADS, 8, tokens), F32),
            pltpu.VMEM((2, width // 128, rows * 8, 128), F32),
            pltpu.VMEM((rows, width), BF),
            pltpu.VMEM((rows, width), BF),
            eight, eight, eight, eight,
            pltpu.SemaphoreType.DMA((len(inputs),)),
        ],
        compiler_params=pltpu.CompilerParams(
            collective_id=0, has_side_effects=True, vmem_limit_bytes=VMEM_LIMIT,
        ),
        name="layer",
    )(*inputs)
    return final.reshape(rows, cols, width), row.reshape(2, cols, width), col, corner


def conv_kernel(final_ref, row_h, col_h, cor_h, weight_ref, image_hbm, image_ref, fb_s, wp_s, up_s, sem):
    rows, cols, width = final_ref.shape
    tokens = rows * cols
    outs = weight_ref.shape[1]
    old = lax.broadcasted_iota(jnp.int32, (outs, outs), 0)
    new = lax.broadcasted_iota(jnp.int32, (outs, outs), 1)
    want = (new % (outs // SHUF)) * SHUF + new // (outs // SHUF)
    perm = jnp.where(old == want, 1.0, 0.0).astype(BF)
    for tap in range(9):
        sl = slice(tap * width, (tap + 1) * width)
        wp_s[sl, :] = jnp.dot(weight_ref[sl, :], perm, preferred_element_type=F32).astype(BF)
    col = lax.broadcasted_iota(jnp.int32, (1, cols, 1), 1)

    def spread(first, count, x, before, after):
        flat = x.reshape(count * cols, width)
        low = pltpu.roll(flat, 1, 0).reshape(count, cols, width)
        high = pltpu.roll(flat, count * cols - 1, 0).reshape(count, cols, width)
        fb_s[1, first : first + count] = x.astype(BF)
        fb_s[0, first : first + count] = jnp.where(col == 0, before, low).astype(BF)
        fb_s[2, first : first + count] = jnp.where(col == cols - 1, after, high).astype(BF)

    for r in range(0, rows, 8):
        before = col_h[0, r : r + 8, :].astype(F32)[:, None, :]
        after = col_h[1, r : r + 8, :].astype(F32)[:, None, :]
        spread(1 + r, 8, final_ref[r : r + 8].astype(F32), before, after)
    for side, at, pick in ((0, 0, 7), (1, rows + 1, 0)):
        before = cor_h[2 * side].astype(F32)[pick : pick + 1][:, None, :]
        after = cor_h[2 * side + 1].astype(F32)[pick : pick + 1][:, None, :]
        spread(at, 1, row_h[side].astype(F32)[None], before, after)

    step = 8
    quarter = outs // SHUF
    outs_going = []
    for r in range(0, rows, step):
        acc = jnp.zeros((step * cols, outs), F32)
        for a in range(3):
            for b in range(3):
                tap = a * 3 + b
                acc = acc + jnp.dot(
                    fb_s[b, r + a : r + a + step].reshape(step * cols, width),
                    wp_s[tap * width : (tap + 1) * width, :],
                    preferred_element_type=F32,
                )
        for k in range(step):
            part = acc[k * cols : (k + 1) * cols]
            slot = k % 2
            for j in range(SHUF):
                pair = j * quarter // 128
                up_s[slot, pl.ds(j, cols, stride=SHUF), :] = part[:, pair * 128 : pair * 128 + 128]
            t = up_s[slot].T
            lanes = lax.broadcasted_iota(jnp.int32, (1, cols * SHUF), 1)
            t = jnp.where(lanes % 2 == 0, t[:quarter], t[quarter : 2 * quarter])
            for c in range(quarter // SHUF):
                image_ref[c, (r + k) * SHUF : (r + k + 1) * SHUF, :] = t[c * SHUF : (c + 1) * SHUF]
        band = pl.ds(r * SHUF, step * SHUF)
        outs_going.append(pltpu.make_async_copy(
            image_ref.at[:, band], image_hbm.at[:, band], sem.at[r // step]
        ))
        outs_going[-1].start()
    for going in outs_going:
        going.wait()


def conv_image(final, row, col, corner, weight):
    rows, cols, width = final.shape
    outs = weight.shape[1]
    vm = pl.BlockSpec(memory_space=pltpu.VMEM)
    return pl.pallas_call(
        conv_kernel,
        out_shape=jax.ShapeDtypeStruct((outs // SHUF**2, rows * SHUF, cols * SHUF), F32),
        in_specs=[vm] * 5,
        out_specs=pl.BlockSpec(memory_space=pltpu.HBM),
        scratch_shapes=[
            pltpu.VMEM((outs // SHUF**2, rows * SHUF, cols * SHUF), F32),
            pltpu.VMEM((3, rows + 2, cols, width), BF),
            pltpu.VMEM(weight.shape, BF),
            pltpu.VMEM((2, cols * SHUF, 128), F32),
            pltpu.SemaphoreType.DMA((rows // 8,)),
        ],
        compiler_params=pltpu.CompilerParams(vmem_limit_bytes=VMEM_LIMIT),
        name="conv_image",
    )(final, row, col, corner, weight)


def local(sizes, field, gains, w_query, w_key, w_value, w_out, w_up, w_down, final_gain, conv_weight):
    final, row, col, corner = layer(
        sizes, field, gains[0], w_query[0], w_key[0], w_value[0], w_out[0], w_up[0], w_down[0],
        final_gain[None, :],
    )
    weight = conv_weight.reshape(-1, conv_weight.shape[3])
    return conv_image(final, row, col, corner, weight)


def solution(mesh):
    sizes = (mesh.shape["row"], mesh.shape["col"])
    return jax.shard_map(
        functools.partial(local, sizes),
        mesh=mesh,
        in_specs=(P("row", "col", None), P(), P(), P(), P(), P(), P(), P(), P(), P()),
        out_specs=P(None, "row", "col"),
        check_vma=False,
    )
```
